32 devices in a mesh: row: 8 (over z, core), col: 4 (over y, x).
Axes of the slice: x: 2, y: 2, z: 4, core: 2. Of those that a mesh axis runs over, the one named last changes fastest.
Arguments:
- blocks: bfloat16 [128, 8, 256, 256], P('row', 'col'), may hold values from -0.125 to 0.125
- block_cols: int32 [128, 8], P('row', 'col'), may hold values from 0 to 48, as said below
- objective: float32 [49152], P(('col', 'row')), may hold values from -6 to 6
- lower_bound: float32 [49152], P(('col', 'row')), may hold values from -1 to -0.2
- upper_bound: float32 [49152], P(('col', 'row')), may hold values from 0.2 to 1
- right_side: float32 [32768], P(('row', 'col')), may hold values from -6 to 6
- primal_init: float32 [49152], P(('col', 'row')), may hold values from -0.2 to 0.2
- dual_init: float32 [32768], P(('row', 'col')), may hold values from 0 to 1
Outputs:
- primal_final: float32 [49152], P(('col', 'row'))
- dual_final: float32 [32768], P(('row', 'col'))
- step_norms: float32 [8, 2], replicated
The draws below stay inside these ranges and needn't reach their ends.
Inputs may be any that keep to these rules, and one draw needn't show every extreme that they name: `block_cols`: entry j of a row block indexes column group j // 2; its live entries (below 48) are distinct within one row block and group, 48 marks an empty slot, and in every draw some row block has all 2 slots of some group live.
All inputs are finite; a program needn't handle non-finite values.
Results may differ from the reference program's by a relative error of at most 0.0015.
Values may be sent and summed in bfloat16 or wider, within the bound.
No kernel may reach another device: no remote copies, remote signals or barrier semaphores. Data moves between devices by JAX's collectives and lax.ppermute only.
A program may use at most 64 MiB of HBM per device.

```python
import jax
import jax.numpy as jnp
from jax import lax

BLOCK = 256
ROW_BLK = 16
COL_BLK = 48
SLOTS = 2
ITERS = 8
ROW_BLOCKS = 128
ROWS = 32768
COLS = 49152
N_ROW = 8
N_COL = 4


def draw_block_cols(key, part):
    row_total = ROW_BLK * N_ROW
    group_total = N_COL
    key_perm = jax.random.fold_in(key, 11)
    key_live = jax.random.fold_in(key, 23)
    key_place = jax.random.fold_in(key, 37)
    perm_keys = jax.random.split(key_perm, row_total * group_total)
    picked_cols = jax.vmap(lambda single: jax.random.permutation(single, COL_BLK)[:SLOTS])(perm_keys)
    picked_cols = picked_cols.reshape(row_total, group_total, SLOTS).astype(jnp.int32)
    live_count = jax.random.randint(key_live, (row_total, group_total), 0, SLOTS + 1)
    place_row = jax.random.randint(key_place, (), 0, row_total)
    place_group = jax.random.randint(jax.random.fold_in(key_place, 5), (), 0, group_total)
    forced = (jnp.arange(row_total, dtype=jnp.int32)[:, None] == place_row) & (jnp.arange(group_total, dtype=jnp.int32)[None, :] == place_group)
    live_count = jnp.where(forced, SLOTS, live_count)
    slot_index = jnp.arange(SLOTS, dtype=jnp.int32)[None, None, :]
    result = jnp.where(slot_index < live_count[:, :, None], picked_cols, COL_BLK)
    return result.reshape(row_total, group_total * SLOTS).astype(jnp.int32)


def block_levels(key, shape, pieces, low, top_value):
    level = 1.0
    for dim, blocks in pieces:
        steps = jax.random.uniform(jax.random.fold_in(jax.random.fold_in(key, 6), dim), (blocks,), jnp.float32, low / len(pieces), top_value / len(pieces))
        level = level * jnp.repeat(jnp.exp(steps), shape[dim] // blocks).reshape((-1,) + (1,) * (len(shape) - 1 - dim))
    return level


def centred(stream_key, shape, deviation, most, cuts=(), kind=jnp.bfloat16):
    loudness = block_levels(stream_key, shape, cuts, -0.22, 0.18) if cuts else 1.0
    values = jax.random.normal(stream_key, shape, jnp.float32) * deviation * loudness
    return jnp.minimum(jnp.maximum(values, -most), most).astype(kind)


def setup_inputs(seed: int = 0) -> dict:
    arg_keys = jax.random.split(jax.random.key(seed), 9)
    return {
        "blocks": centred(arg_keys[0], (ROW_BLOCKS, N_COL * SLOTS, BLOCK, BLOCK), (BLOCK * SLOTS * N_COL) ** -0.5, 0.125, ((0, 8), (1, 4))),
        "block_cols": draw_block_cols(jax.random.fold_in(arg_keys[8], 71), 0),
        "objective": centred(arg_keys[2], (COLS,), 1.0, 6.0, ((0, 32),), jnp.float32),
        "lower_bound": jnp.clip(-1.0 + 0.8 * jax.random.uniform(arg_keys[3], (COLS,), jnp.float32) ** block_levels(arg_keys[3], (COLS,), ((0, 32),), -0.2, 0.2), -1.0, -0.2),
        "upper_bound": jnp.clip(0.2 + 0.8 * jax.random.uniform(arg_keys[4], (COLS,), jnp.float32) ** block_levels(arg_keys[4], (COLS,), ((0, 32),), -0.2, 0.2), 0.2, 1.0),
        "right_side": centred(arg_keys[5], (ROWS,), 1.0, 6.0, ((0, 32),), jnp.float32),
        "primal_init": jnp.clip(jax.random.uniform(arg_keys[6], (COLS,), jnp.float32, -0.2, 0.2) * block_levels(arg_keys[6], (COLS,), ((0, 32),), -0.4, 0.0), -0.2, 0.2),
        "dual_init": jnp.clip(1.0 * jax.random.uniform(arg_keys[7], (ROWS,), jnp.float32) ** block_levels(arg_keys[7], (ROWS,), ((0, 32),), -0.2, 0.2), 0.0, 1.0),
    }


step_primal = 0.5
step_dual = 0.5

def reference(blocks, block_cols, objective, lower_bound, upper_bound, right_side, primal_init, dual_init):
    total_blocks = blocks.shape[0]
    slot_total = blocks.shape[1]
    width = blocks.shape[2]
    col_total = COL_BLK * N_COL
    live = block_cols < COL_BLK
    group = jnp.arange(slot_total, dtype=jnp.int32) // SLOTS
    indices = jnp.where(live, group[None, :] * COL_BLK + block_cols, 0).astype(jnp.int32)
    weight_mask = live.astype(jnp.float32)
    grouped_blocks = blocks.reshape(N_ROW, total_blocks // N_ROW, slot_total, width, width)
    grouped_idx = indices.reshape(N_ROW, total_blocks // N_ROW, slot_total)
    grouped_mask = weight_mask.reshape(N_ROW, total_blocks // N_ROW, slot_total)

    def times_matrix(vector_half):
        lookup = vector_half.astype(jnp.float32).reshape(col_total, width)

        def one_group(packed):
            block_group, index_group, mask_group = packed
            picked = lookup[index_group] * mask_group[:, :, None]
            return jnp.einsum('gjab,gjb->ga', block_group.astype(jnp.float32), picked, precision=lax.Precision.HIGHEST)
        return lax.map(one_group, (grouped_blocks, grouped_idx, grouped_mask)).reshape(-1)

    def times_transpose(vector_half):
        values = vector_half.astype(jnp.float32).reshape(N_ROW, total_blocks // N_ROW, width)

        def one_group(packed):
            block_group, value_group, mask_group = packed
            contrib = jnp.einsum('gjab,ga->gjb', block_group.astype(jnp.float32), value_group, precision=lax.Precision.HIGHEST)
            return contrib * mask_group[:, :, None]
        contrib = lax.map(one_group, (grouped_blocks, values, grouped_mask))
        summed = jax.ops.segment_sum(contrib.reshape(-1, width), indices.reshape(-1), num_segments=col_total)
        return summed.reshape(-1)
    primal_now = primal_init
    dual_now = dual_init
    history = []
    for iteration in range(ITERS):
        dual_half = dual_now.astype(jnp.bfloat16)
        gradient = times_transpose(dual_half)
        primal_next = jnp.minimum(upper_bound, jnp.maximum(lower_bound, primal_now - step_primal * (objective - gradient)))
        extrapolated = (2.0 * primal_next - primal_now).astype(jnp.bfloat16)
        image_dual = times_matrix(extrapolated)
        dual_next = jnp.maximum(dual_now + step_dual * (right_side - image_dual), 0.0)
        primal_step = primal_next - primal_now
        dual_step = dual_next - dual_now
        history.append(jnp.stack((jnp.sqrt(jnp.mean(primal_step * primal_step)), jnp.sqrt(jnp.mean(dual_step * dual_step)))))
        primal_now = primal_next
        dual_now = dual_next
    return (primal_now, dual_now, jnp.stack(history))
```

```python
import functools

import jax
import jax.numpy as jnp
from jax import lax
from jax.experimental import pallas as pl
from jax.experimental.pallas import tpu as pltpu
from jax.sharding import PartitionSpec as P

ITERS = 8
STEP_PRIMAL = 0.5
STEP_DUAL = 0.5
PAD = 8

F32 = jnp.float32
BF16 = jnp.bfloat16


def is_dual_core():
    return lax.axis_index("row") % 2 == 0


def assemble(ref, parts, first, rows, stride, me):
    for j in range(len(parts)):
        piece = parts[0]
        for o in range(1, len(parts)):
            piece = jnp.where(me == (j ^ o), parts[o], piece)
        ref[pl.ds(first + j * stride, rows), :] = piece


def total_of(refs, rows):
    total = refs[0][pl.ds(0, rows), :]
    for ref in refs[1:]:
        total = total + ref[pl.ds(0, rows), :]
    return total


def dual_body(iteration, last, n_msgs, slots, *refs):
    msgs = refs[:n_msgs]
    (dual_ref, hist_ref, cost_ref, one_ref, mine_ref, theirs_ref) = refs[n_msgs : n_msgs + 6]
    (out_ref, dual_out, hist_out, prod_ref) = refs[n_msgs + 6 :]
    rows = dual_out.shape[0]
    blocks = cost_ref.shape[0]

    @pl.when(is_dual_core())
    def _():
        if iteration == 0:
            each = rows // (2 * n_msgs)
            me = lax.axis_index("col")
            for slab in range(2):
                parts = [m[pl.ds(slab * each, each), :] for m in msgs]
                assemble(dual_out, parts, slab * (rows // 2), each, each, me)
            dual_next = dual_out[...]
            norm = jnp.zeros((1, dual_next.shape[1]), F32)
            hist_out[...] = jnp.zeros_like(hist_out)
        else:
            total = total_of(msgs, rows + PAD)
            dual = dual_ref[...]
            dual_next = jnp.maximum(dual - STEP_DUAL * total[:rows], 0.0)
            step = dual_next - dual
            norm = jnp.sum(step * step, axis=0, keepdims=True)
            dual_out[...] = dual_next
            hist_out[...] = hist_ref[...]
            hist_out[pl.ds(iteration - 1, 1), :] = total[rows : rows + 1]
        if last:
            out_ref[...] = jnp.zeros_like(out_ref)
            out_ref[pl.ds(0, 1), :] = norm
            return
        half = dual_next.astype(BF16)
        for slab, blk_ref in enumerate((mine_ref, theirs_ref)):
            for b in range(blk_ref.shape[0]):
                e = slab * blk_ref.shape[0] + b
                r = e // slots
                prod_ref[pl.ds(e, 1), :] = jnp.dot(
                    half[r : r + 1], blk_ref[b], preferred_element_type=F32
                )
        prod = prod_ref[...]
        high = prod.astype(BF16)
        rest = prod - high.astype(F32)
        mid = rest.astype(BF16)
        low = (rest - mid.astype(F32)).astype(BF16)
        stacked = jnp.concatenate([high, mid, low], axis=0)
        grad = jnp.dot(one_ref[...], stacked, preferred_element_type=F32)
        out_ref[pl.ds(0, blocks), :] = grad - cost_ref[...]
        out_ref[pl.ds(blocks, PAD), :] = jnp.concatenate(
            [norm, jnp.zeros((PAD - 1, norm.shape[1]), F32)], axis=0
        )


def primal_body(iteration, n_msgs, slots, *refs):
    msgs = refs[:n_msgs]
    (primal_ref, low_ref, up_ref, hist_ref, right_ref, pick_ref, mine_ref, theirs_ref) = refs[
        n_msgs : n_msgs + 8
    ]
    (out_ref, primal_out, low_out, up_out, hist_out) = refs[n_msgs + 8 : n_msgs + 13]
    blocks = primal_out.shape[0]
    rows = right_ref.shape[0]

    @pl.when(jnp.logical_not(is_dual_core()))
    def _():
        total = total_of(msgs, blocks + PAD)
        if iteration == 0:
            each = blocks // n_msgs
            me = lax.axis_index("row") // 2
            for k, ref in enumerate((primal_out, low_out, up_out)):
                parts = [m[pl.ds(blocks + PAD + k * each, each), :] for m in msgs]
                assemble(ref, parts, 0, each, each, me)
            primal, low, up = primal_out[...], low_out[...], up_out[...]
            hist_out[...] = jnp.zeros_like(hist_out)
        else:
            primal, low, up = primal_ref[...], low_ref[...], up_ref[...]
            low_out[...] = low
            up_out[...] = up
            hist_out[...] = hist_ref[...]
            hist_out[pl.ds(iteration - 1, 1), :] = total[blocks : blocks + 1]
        primal_next = jnp.minimum(up, jnp.maximum(low, primal + STEP_PRIMAL * total[:blocks]))
        step = primal_next - primal
        norm = jnp.sum(step * step, axis=0, keepdims=True)
        primal_out[...] = primal_next
        ext = (2.0 * primal_next - primal).astype(BF16)
        picked = jnp.dot(pick_ref[...], ext, preferred_element_type=F32).astype(BF16)
        for slab, blk_ref in enumerate((theirs_ref, mine_ref)):
            for r in range(blk_ref.shape[0] // slots):
                acc = None
                for s in range(slots):
                    b = r * slots + s
                    e = slab * blk_ref.shape[0] + b
                    term = lax.dot_general(
                        picked[e : e + 1],
                        blk_ref[b],
                        (((1,), (1,)), ((), ())),
                        preferred_element_type=F32,
                    )
                    acc = term if acc is None else acc + term
                row = slab * (rows // 2) + r
                out_ref[pl.ds(row, 1), :] = acc - right_ref[pl.ds(row, 1), :]
        out_ref[pl.ds(rows, PAD), :] = jnp.concatenate(
            [norm, jnp.zeros((PAD - 1, norm.shape[1]), F32)], axis=0
        )


def local_call(body, outs, scratch, n_in):
    return pl.pallas_call(
        body,
        out_shape=outs,
        in_specs=[pl.BlockSpec(memory_space=pltpu.VMEM)] * n_in,
        out_specs=[pl.BlockSpec(memory_space=pltpu.VMEM)] * len(outs),
        scratch_shapes=scratch,
        compiler_params=pltpu.CompilerParams(vmem_limit_bytes=24 * 2**20),
    )


def per_device(
    blocks, block_cols, objective, lower_bound, upper_bound, right_side, primal_init, dual_init
):
    slab_rows, slots, width = blocks.shape[0], blocks.shape[1], blocks.shape[2]
    n_row, n_col = lax.axis_size("row"), lax.axis_size("col")
    n_z = n_row // 2
    p_rows = primal_init.shape[0] // width
    d_rows = dual_init.shape[0] // width
    col_blocks = p_rows * n_row
    rows = 2 * slab_rows
    row, col = lax.axis_index("row"), lax.axis_index("col")
    core, z = row % 2, row // 2
    is_dual = core == 0

    swap_pairs = [(r, r ^ 1) for r in range(n_row)]

    def over_z(src, o):
        away = [(2 * k + src, 2 * (k ^ o) + 1 - src) for k in range(n_z)]
        return away + [(2 * k + 1 - src, 2 * k + src) for k in range(n_z)]

    def over_col(src, o):
        pairs = []
        for k in range(n_z):
            for c in range(n_col):
                pairs.append(((2 * k + src) * n_col + c, (2 * k + 1 - src) * n_col + (c ^ o)))
                pairs.append(((2 * k + 1 - src) * n_col + c, (2 * k + src) * n_col + c))
        return pairs

    def to_primal(x):
        return [lax.ppermute(x, "row", over_z(0, o)) for o in range(n_z)]

    def to_dual(x):
        return [lax.ppermute(x, ("row", "col"), over_col(1, o)) for o in range(n_col)]

    own = jnp.concatenate(
        [
            dual_init.reshape(d_rows, width),
            right_side.reshape(d_rows, width),
            objective.reshape(p_rows, width),
            primal_init.reshape(p_rows, width),
            lower_bound.reshape(p_rows, width),
            upper_bound.reshape(p_rows, width),
            jnp.pad(
                block_cols.astype(F32).reshape(-1, slab_rows * slots),
                ((0, 0), (0, width - slab_rows * slots)),
            ),
        ],
        axis=0,
    )
    other = lax.ppermute(own, "row", swap_pairs)
    mine = blocks.reshape(slab_rows * slots, width, width)
    theirs = lax.ppermute(mine, "row", swap_pairs)
    first = jnp.where(is_dual, own, other)
    second = jnp.where(is_dual, other, own)

    def both(lo, n):
        return jnp.concatenate([first[lo : lo + n], second[lo : lo + n]], axis=0)

    at = 0
    parts = []
    for n in (d_rows, d_rows, p_rows, p_rows, p_rows, p_rows):
        parts.append(both(at, n))
        at += n
    dual_part, right_part, cost_part, primal_part, low_part, up_part = parts
    cols = both(at, 1)[:, : slab_rows * slots].reshape(1, -1)
    one_hot = (cols == jnp.arange(col_blocks, dtype=F32)[:, None]).astype(BF16)
    one_three = jnp.concatenate([one_hot] * 3, axis=1)
    pick = one_hot.T
    cost = lax.dynamic_update_slice_in_dim(
        jnp.zeros((col_blocks, width), F32), cost_part, z * 2 * p_rows, 0
    )
    right = jnp.zeros((rows, width), F32)
    for slab in range(2):
        right = lax.dynamic_update_slice_in_dim(
            right,
            right_part[slab * d_rows : (slab + 1) * d_rows],
            slab * slab_rows + col * d_rows,
            0,
        )

    def shape(n, dtype=F32):
        return jax.ShapeDtypeStruct((n, width), dtype)

    hist_rows = -(-ITERS // 8) * 8
    dual = jnp.zeros((rows, width), F32)
    primal_hist = jnp.zeros((hist_rows, width), F32)
    dual_hist = primal_hist
    primal = low = up = jnp.zeros((col_blocks, width), F32)
    products = pltpu.VMEM((2 * slab_rows * slots, width), F32)

    arrived = to_dual(dual_part)
    for iteration in range(ITERS):
        message, dual, primal_hist = local_call(
            functools.partial(dual_body, iteration, False, n_col, slots),
            [shape(col_blocks + PAD), shape(rows), shape(hist_rows)],
            [products],
            n_col + 6,
        )(*arrived, dual, primal_hist, cost, one_three, mine, theirs)
        if iteration == 0:
            message = jnp.concatenate([message, primal_part, low_part, up_part], axis=0)
        arrived = to_primal(message)
        message, primal, low, up, dual_hist = local_call(
            functools.partial(primal_body, iteration, n_z, slots),
            [shape(rows + PAD), shape(col_blocks), shape(col_blocks), shape(col_blocks), shape(hist_rows)],
            [],
            n_z + 8,
        )(*arrived, primal, low, up, dual_hist, right, pick, mine, theirs)
        arrived = to_dual(message)
    message, dual, primal_hist = local_call(
        functools.partial(dual_body, ITERS, True, n_col, slots),
        [shape(PAD), shape(rows), shape(hist_rows)],
        [products],
        n_col + 6,
    )(*arrived, dual, primal_hist, cost, one_three, mine, theirs)

    send_rows = max(p_rows, d_rows)
    dual_away = lax.dynamic_slice_in_dim(dual, slab_rows + col * d_rows, d_rows, 0)
    primal_away = lax.dynamic_slice_in_dim(primal, z * 2 * p_rows, p_rows, 0)
    away = jnp.where(
        is_dual,
        jnp.pad(dual_away, ((0, send_rows - d_rows), (0, 0))),
        jnp.pad(primal_away, ((0, send_rows - p_rows), (0, 0))),
    )
    back = lax.ppermute(away, "row", swap_pairs)
    dual_mine = lax.dynamic_slice_in_dim(dual, col * d_rows, d_rows, 0)
    primal_mine = lax.dynamic_slice_in_dim(primal, z * 2 * p_rows + p_rows, p_rows, 0)
    dual_out = jnp.where(is_dual, dual_mine, back[:d_rows]).reshape(-1)
    primal_out = jnp.where(is_dual, back[:p_rows], primal_mine).reshape(-1)

    arrived = to_primal(jnp.concatenate([message, primal_hist], axis=0))
    last_dual = sum(a[:1] for a in arrived)
    primal_sq = jnp.sum(arrived[0][PAD : PAD + ITERS], axis=1)
    dual_sq = jnp.sum(
        lax.dynamic_update_slice_in_dim(dual_hist, last_dual, ITERS - 1, 0)[:ITERS], axis=1
    )
    totals = jnp.array(
        [float(primal_init.shape[0] * n_row * n_col), float(dual_init.shape[0] * n_row * n_col)], F32
    )
    norms = jnp.sqrt(jnp.stack([primal_sq, dual_sq], axis=1) / totals[None, :])
    norms = jnp.where(is_dual, lax.ppermute(norms, "row", swap_pairs), norms)
    return (primal_out, dual_out, norms)


def solution(mesh):
    in_specs = (
        P("row", "col", None, None),
        P("row", "col"),
        P(("col", "row")),
        P(("col", "row")),
        P(("col", "row")),
        P(("row", "col")),
        P(("col", "row")),
        P(("row", "col")),
    )
    out_specs = (P(("col", "row")), P(("row", "col")), P())
    return jax.shard_map(
        per_device, mesh=mesh, in_specs=in_specs, out_specs=out_specs, check_vma=False
    )
```

```python
import functools

import jax
import jax.numpy as jnp
from jax import lax
from jax.experimental import pallas as pl
from jax.experimental.pallas import tpu as pltpu
from jax.sharding import PartitionSpec as P

ITERS = 8
STEP_PRIMAL = 0.5
STEP_DUAL = 0.5
PAD = 8

F32 = jnp.float32
BF16 = jnp.bfloat16


def is_dual_core():
    return lax.axis_index("row") % 2 == 0


def assemble(ref, parts, first, rows, stride, me):
    for j in range(len(parts)):
        piece = parts[0]
        for o in range(1, len(parts)):
            piece = jnp.where(me == (j ^ o), parts[o], piece)
        ref[pl.ds(first + j * stride, rows), :] = piece


def by_offset(refs, order):
    return [refs[order.index(o)] for o in range(len(order))]


def total_of(refs, rows):
    level = [ref[pl.ds(0, rows), :] for ref in refs]
    while len(level) > 1:
        level = [level[i] + level[i + 1] for i in range(0, len(level), 2)]
    return level[0]


def z_order(n):
    return [3, 1, 2, 0] if n == 4 else list(range(n))


def col_order(n):
    return [3, 1, 2, 0] if n == 4 else list(range(n))


def update_dual(iteration, msgs, dual_ref, hist_ref, dual_out, hist_out):
    rows = dual_out.shape[0]
    total = total_of(msgs, rows + PAD)
    dual = dual_ref[...]
    dual_next = jnp.maximum(dual - STEP_DUAL * total[:rows], 0.0)
    step = dual_next - dual
    dual_out[...] = dual_next
    hist_out[...] = hist_ref[...]
    hist_out[pl.ds(iteration - 1, 1), :] = total[rows : rows + 1]
    return dual_next, jnp.sum(step * step, axis=0, keepdims=True)


def dual_body(iteration, n_msgs, slots, *refs):
    msgs = by_offset(refs[:n_msgs], col_order(n_msgs))
    (dual_ref, hist_ref, cost_ref, one_ref, extra_ref, *blk_refs) = refs[n_msgs : n_msgs + 7]
    (out_ref, dual_out, hist_out, prod_ref) = refs[n_msgs + 7 :]
    rows, width = dual_out.shape
    blocks = cost_ref.shape[0]

    @pl.when(is_dual_core())
    def _():
        if iteration == 0:
            each = rows // (2 * n_msgs)
            me = lax.axis_index("col")
            for slab in range(2):
                parts = [m[pl.ds(slab * each, each), :] for m in msgs]
                assemble(dual_out, parts, slab * (rows // 2), each, each, me)
            dual_next = dual_out[...]
            norm = jnp.zeros((1, width), F32)
            hist_out[...] = jnp.zeros_like(hist_out)
            out_ref[pl.ds(blocks + PAD, extra_ref.shape[0]), :] = extra_ref[...]
        else:
            dual_next, norm = update_dual(iteration, msgs, dual_ref, hist_ref, dual_out, hist_out)
        half = dual_next.astype(BF16)
        slab_rows = rows // 2
        for r in range(rows):
            for s in range(slots):
                at = (r // slab_rows * slots + s) * slab_rows + r % slab_rows
                prod_ref[pl.ds(at, 1), :] = jnp.dot(
                    half[r : r + 1], blk_refs[r // slab_rows][r % slab_rows * slots + s], preferred_element_type=F32
                )
        prod = prod_ref[...]
        high = prod.astype(BF16)
        rest = prod - high.astype(F32)
        mid = rest.astype(BF16)
        low = (rest - mid.astype(F32)).astype(BF16)
        stacked = jnp.concatenate([high, mid, low], axis=0)
        grad = jnp.dot(one_ref[...], stacked, preferred_element_type=F32)
        out_ref[pl.ds(0, blocks), :] = grad - cost_ref[...]
        out_ref[pl.ds(blocks, PAD), :] = jnp.concatenate(
            [norm, jnp.zeros((PAD - 1, width), F32)], axis=0
        )


def take(ref, index, count, first, rows, stride):
    piece = ref[pl.ds(first, rows), :]
    for j in range(1, count):
        piece = jnp.where(index == j, ref[pl.ds(first + j * stride, rows), :], piece)
    return piece


def last_body(iterations, n_msgs, d_rows, p_rows, n_z, *refs):
    msgs = by_offset(refs[:n_msgs], col_order(n_msgs))
    (dual_ref, hist_ref, primal_ref) = refs[n_msgs : n_msgs + 3]
    (out_ref, dual_out, away_ref) = refs[n_msgs + 3 :]
    half = dual_out.shape[0] // 2
    dual_core = is_dual_core()

    @pl.when(dual_core)
    def _():
        hist_out = out_ref.at[pl.ds(PAD, hist_ref.shape[0])]
        _, norm = update_dual(iterations, msgs, dual_ref, hist_ref, dual_out, hist_out)
        out_ref[pl.ds(0, PAD), :] = jnp.concatenate(
            [norm, jnp.zeros((PAD - 1, norm.shape[1]), F32)], axis=0
        )
        away_ref[pl.ds(0, d_rows), :] = take(
            dual_out, lax.axis_index("col"), n_msgs, half, d_rows, d_rows
        )

    @pl.when(jnp.logical_not(dual_core))
    def _():
        away_ref[pl.ds(0, p_rows), :] = take(
            primal_ref, lax.axis_index("row") // 2, n_z, 0, p_rows, 2 * p_rows
        )


def finish_body(iterations, n_msgs, n_col, p_total, d_total, *refs):
    msgs = by_offset(refs[:n_msgs], z_order(n_msgs))
    (hist_ref, dual_ref, primal_ref, back_ref) = refs[n_msgs : n_msgs + 4]
    (primal_out, dual_out, norm_out, keep_ref) = refs[n_msgs + 4 :]
    width = dual_ref.shape[1]
    d_rows, p_rows = dual_out.shape[0] // width, primal_out.shape[0] // width
    dual_core = is_dual_core()

    def give(out_ref, rows):
        for r in range(rows.shape[0]):
            out_ref[pl.ds(r * width, width)] = rows[r]

    @pl.when(dual_core)
    def _():
        give(dual_out, take(dual_ref, lax.axis_index("col"), n_col, 0, d_rows, d_rows))
        give(primal_out, back_ref[pl.ds(0, p_rows), :])

    @pl.when(jnp.logical_not(dual_core))
    def _():
        give(dual_out, back_ref[pl.ds(0, d_rows), :])
        give(
            primal_out,
            take(primal_ref, lax.axis_index("row") // 2, n_msgs, p_rows, p_rows, 2 * p_rows),
        )
        last = total_of(msgs, 1)
        keep_ref[...] = hist_ref[...]
        keep_ref[pl.ds(iterations - 1, 1), :] = last
        primal_sq = jnp.sum(msgs[0][pl.ds(PAD, hist_ref.shape[0]), :], axis=1, keepdims=True)
        dual_sq = jnp.sum(keep_ref[...], axis=1, keepdims=True)
        lane = lax.broadcasted_iota(jnp.int32, norm_out.shape, 1)
        norm_out[...] = jnp.sqrt(
            jnp.where(lane == 0, primal_sq * (1.0 / p_total), dual_sq * (1.0 / d_total))
        )


def pack_body(n, *refs):
    (sources, out_ref, held, sem) = (refs[:n], refs[n], refs[n + 1 : 2 * n + 1], refs[2 * n + 1])
    copies = [
        pltpu.make_async_copy(source, ref, sem.at[i])
        for i, (source, ref) in enumerate(zip(sources, held, strict=True))
    ]
    for copy in copies:
        copy.start()
    for copy in copies:
        copy.wait()
    (cols_ref, *vectors) = held
    width = out_ref.shape[1]
    at = 0
    for ref in vectors:
        for i in range(ref.shape[0] // width):
            out_ref[at, :] = ref[pl.ds(i * width, width)]
            at += 1
    out_ref[pl.ds(at, cols_ref.shape[0]), pl.ds(0, cols_ref.shape[1])] = cols_ref[...].astype(F32)


def pack_call(out, *arrays):
    n = len(arrays)
    return pl.pallas_call(
        functools.partial(pack_body, n),
        out_shape=out,
        in_specs=[pl.BlockSpec(memory_space=pltpu.HBM)] * n,
        out_specs=pl.BlockSpec(memory_space=pltpu.VMEM),
        scratch_shapes=[pltpu.VMEM(a.shape, a.dtype) for a in arrays]
        + [pltpu.SemaphoreType.DMA((n,))],
        compiler_params=pltpu.CompilerParams(vmem_limit_bytes=4 * 2**20),
    )(*arrays)


def setup_body(d_rows, p_rows, slab_rows, slots, n_z, n_col, *refs):
    (own_ref, other_ref, dual_out, extra_out, cost_out, right_out, one_out, pick_out) = refs
    dual_core = is_dual_core()
    first = jnp.where(dual_core, own_ref[...], other_ref[...])
    second = jnp.where(dual_core, other_ref[...], own_ref[...])
    z, col = lax.axis_index("row") // 2, lax.axis_index("col")
    at = 0
    for slab, part in enumerate((first, second)):
        dual_out[pl.ds(slab * d_rows, d_rows), :] = part[:d_rows]
    at += d_rows
    for slab, part in enumerate((first, second)):
        piece = part[at : at + d_rows]
        for j in range(n_col):
            right_out[pl.ds(slab * slab_rows + j * d_rows, d_rows), :] = jnp.where(
                col == j, piece, 0.0
            )
    at += d_rows
    for slab, part in enumerate((first, second)):
        piece = part[at : at + p_rows]
        for j in range(n_z):
            cost_out[pl.ds((2 * j + slab) * p_rows, p_rows), :] = jnp.where(z == j, piece, 0.0)
    at += p_rows
    for k in range(3):
        for slab, part in enumerate((first, second)):
            extra_out[pl.ds((2 * k + slab) * p_rows, p_rows), :] = part[at : at + p_rows]
        at += p_rows
    entries, blocks = pick_out.shape
    columns = [
        part[at : at + slab_rows, s : s + 1] for part in (first, second) for s in range(slots)
    ]
    side = -(-entries // 128) * 128
    columns.append(jnp.full((side - entries, 1), -1.0, F32))
    column = jnp.concatenate(columns, axis=0)
    lanes = -(-blocks // 128) * 128
    iota = lax.broadcasted_iota(jnp.int32, (side, lanes), 1).astype(F32)
    pick = jnp.where(jnp.broadcast_to(column, (side, lanes)) == iota, 1.0, 0.0)
    pick_out[...] = pick[:entries, :blocks].astype(BF16)
    one = pick.T[:blocks, :entries]
    one_out[...] = jnp.concatenate([one] * 3, axis=1).astype(BF16)


def primal_body(iteration, n_msgs, slots, *refs):
    msgs = by_offset(refs[:n_msgs], z_order(n_msgs))
    (primal_ref, low_ref, up_ref, hist_ref, right_ref, pick_ref, *blk_refs) = refs[
        n_msgs : n_msgs + 8
    ]
    (out_ref, primal_out, low_out, up_out, hist_out) = refs[n_msgs + 8 :]
    blk_refs = blk_refs[::-1]
    blocks = primal_out.shape[0]
    rows = right_ref.shape[0]
    slab_rows = rows // 2

    @pl.when(jnp.logical_not(is_dual_core()))
    def _():
        total = total_of(msgs, blocks + PAD)
        if iteration == 0:
            each = blocks // n_msgs
            me = lax.axis_index("row") // 2
            for k, ref in enumerate((primal_out, low_out, up_out)):
                parts = [m[pl.ds(blocks + PAD + k * each, each), :] for m in msgs]
                assemble(ref, parts, 0, each, each, me)
            primal, low, up = primal_out[...], low_out[...], up_out[...]
            hist_out[...] = jnp.zeros_like(hist_out)
        else:
            primal, low, up = primal_ref[...], low_ref[...], up_ref[...]
            low_out[...] = low
            up_out[...] = up
            hist_out[...] = hist_ref[...]
            hist_out[pl.ds(iteration - 1, 1), :] = total[blocks : blocks + 1]
        primal_next = jnp.minimum(up, jnp.maximum(low, primal + STEP_PRIMAL * total[:blocks]))
        step = primal_next - primal
        norm = jnp.sum(step * step, axis=0, keepdims=True)
        primal_out[...] = primal_next
        ext = (2.0 * primal_next - primal).astype(BF16)
        picked = jnp.dot(pick_ref[...], ext, preferred_element_type=F32).astype(BF16)
        for r in range(rows):
            acc = -right_ref[pl.ds(r, 1), :]
            for s in range(slots):
                at = (r // slab_rows * slots + s) * slab_rows + r % slab_rows
                acc = acc + jnp.dot(
                    picked[at : at + 1],
                    blk_refs[r // slab_rows][r % slab_rows * slots + s],
                    preferred_element_type=F32,
                )
            out_ref[pl.ds(r, 1), :] = acc
        out_ref[pl.ds(rows, PAD), :] = jnp.concatenate(
            [norm, jnp.zeros((PAD - 1, norm.shape[1]), F32)], axis=0
        )


def weights_body(in_ref, out_ref, sem):
    copy = pltpu.make_async_copy(in_ref, out_ref, sem)
    copy.start()
    copy.wait()

    @pl.when(jnp.logical_not(is_dual_core()))
    def _():
        def step(i, carry):
            for k in range(4):
                out_ref[i * 4 + k] = out_ref[i * 4 + k].T
            return carry

        lax.fori_loop(0, in_ref.shape[0] // 4, step, 0)


def weights_call(blocks):
    return pl.pallas_call(
        weights_body,
        out_shape=jax.ShapeDtypeStruct(blocks.shape, BF16),
        in_specs=[pl.BlockSpec(memory_space=pltpu.HBM)],
        out_specs=pl.BlockSpec(memory_space=pltpu.VMEM),
        scratch_shapes=[pltpu.SemaphoreType.DMA],
        compiler_params=pltpu.CompilerParams(vmem_limit_bytes=8 * 2**20),
    )(blocks)


def local_call(body, outs, scratch, n_in):
    return pl.pallas_call(
        body,
        out_shape=outs,
        in_specs=[pl.BlockSpec(memory_space=pltpu.VMEM)] * n_in,
        out_specs=[pl.BlockSpec(memory_space=pltpu.VMEM)] * len(outs),
        scratch_shapes=scratch,
        compiler_params=pltpu.CompilerParams(vmem_limit_bytes=4 * 2**20),
    )


def per_device(
    blocks, block_cols, objective, lower_bound, upper_bound, right_side, primal_init, dual_init
):
    slab_rows, slots, width = blocks.shape[0], blocks.shape[1], blocks.shape[2]
    n_row, n_col = lax.axis_size("row"), lax.axis_size("col")
    n_z = n_row // 2
    p_rows = primal_init.shape[0] // width
    d_rows = dual_init.shape[0] // width
    col_blocks = p_rows * n_row
    rows = 2 * slab_rows
    entries = rows * slots
    is_dual = is_dual_core()

    swap_pairs = [(r, r ^ 1) for r in range(n_row)]

    def over_z(src, o):
        away = [(2 * k + src, 2 * (k ^ o) + 1 - src) for k in range(n_z)]
        return away + [(2 * k + 1 - src, 2 * k + src) for k in range(n_z)]

    def over_col(src, o):
        pairs = []
        for k in range(n_z):
            for c in range(n_col):
                pairs.append(((2 * k + src) * n_col + c, (2 * k + 1 - src) * n_col + (c ^ o)))
                pairs.append(((2 * k + 1 - src) * n_col + c, (2 * k + src) * n_col + c))
        return pairs

    def to_primal(x):
        return [lax.ppermute(x, "row", over_z(0, o)) for o in z_order(n_z)]

    def to_dual(x):
        return [lax.ppermute(x, ("row", "col"), over_col(1, o)) for o in col_order(n_col)]

    def shape(n, wide=width, dtype=F32):
        return jax.ShapeDtypeStruct((n, wide), dtype)

    mine = blocks.reshape(slab_rows * slots, width, width)
    own = pack_call(
        shape(2 * d_rows + 4 * p_rows + slab_rows),
        block_cols, dual_init, right_side, objective, primal_init, lower_bound, upper_bound,
    )
    other = lax.ppermute(own, "row", swap_pairs)
    gated, other = lax.optimization_barrier((mine, other))
    theirs = lax.ppermute(gated, "row", swap_pairs)
    dual_part, extra, cost, right, one_three, pick = local_call(
        functools.partial(setup_body, d_rows, p_rows, slab_rows, slots, n_z, n_col),
        [
            shape(2 * d_rows),
            shape(6 * p_rows),
            shape(col_blocks),
            shape(rows),
            shape(col_blocks, 3 * entries, BF16),
            shape(entries, col_blocks, BF16),
        ],
        [],
        2,
    )(own, other)
    weights = (weights_call(mine), weights_call(theirs))

    hist_rows = -(-ITERS // 8) * 8
    dual = right
    primal = low = up = cost
    primal_hist = dual_hist = jnp.zeros((hist_rows, width), F32)
    products = pltpu.VMEM((entries, width), F32)

    arrived = to_dual(dual_part)
    for iteration in range(ITERS):
        message, dual, primal_hist = local_call(
            functools.partial(dual_body, iteration, n_col, slots),
            [
                shape(col_blocks + PAD + (6 * p_rows if iteration == 0 else 0)),
                shape(rows),
                shape(hist_rows),
            ],
            [products],
            n_col + 7,
        )(*arrived, dual, primal_hist, cost, one_three, extra, *weights)
        arrived = to_primal(message)
        message, primal, low, up, dual_hist = local_call(
            functools.partial(primal_body, iteration, n_z, slots),
            [
                shape(rows + PAD),
                shape(col_blocks),
                shape(col_blocks),
                shape(col_blocks),
                shape(hist_rows),
            ],
            [],
            n_z + 8,
        )(*arrived, primal, low, up, dual_hist, right, pick, *weights)
        arrived = to_dual(message)
    message, dual, away = local_call(
        functools.partial(last_body, ITERS, n_col, d_rows, p_rows, n_z),
        [shape(PAD + hist_rows), shape(rows), shape(max(p_rows, d_rows))],
        [],
        n_col + 3,
    )(*arrived, dual, primal_hist, primal)
    back = lax.ppermute(away, "row", swap_pairs)
    arrived = to_primal(message)
    primal_out, dual_out, norms = local_call(
        functools.partial(
            finish_body,
            ITERS,
            n_z,
            n_col,
            float(primal_init.shape[0] * n_row * n_col),
            float(dual_init.shape[0] * n_row * n_col),
        ),
        [
            jax.ShapeDtypeStruct(primal_init.shape, F32),
            jax.ShapeDtypeStruct(dual_init.shape, F32),
            shape(hist_rows, 2),
        ],
        [pltpu.VMEM((hist_rows, width), F32)],
        n_z + 4,
    )(*arrived, dual_hist, dual, primal, back)
    norms = jnp.where(is_dual, lax.ppermute(norms, "row", swap_pairs), norms)[:ITERS]
    return (primal_out, dual_out, norms)


def solution(mesh):
    in_specs = (
        P("row", "col", None, None),
        P("row", "col"),
        P(("col", "row")),
        P(("col", "row")),
        P(("col", "row")),
        P(("row", "col")),
        P(("col", "row")),
        P(("row", "col")),
    )
    out_specs = (P(("col", "row")), P(("row", "col")), P())
    return jax.shard_map(
        per_device, mesh=mesh, in_specs=in_specs, out_specs=out_specs, check_vma=False
    )
```

```python
import functools

import jax
import jax.numpy as jnp
from jax import lax
from jax.experimental import pallas as pl
from jax.experimental.pallas import tpu as pltpu
from jax.sharding import PartitionSpec as P


ITERS = 8
STEP_PRIMAL = 0.5
STEP_DUAL = 0.5

DUAL = 0

F32 = jnp.float32
BF16 = jnp.bfloat16


def is_dual_core():
    return lax.axis_index("row") % 2 == DUAL


def assemble(ref, parts, first, rows, stride, me):
    for j in range(len(parts)):
        piece = parts[0]
        for o in range(1, len(parts)):
            piece = jnp.where(me == (j ^ o), parts[o], piece)
        ref[pl.ds(first + j * stride, rows), :] = piece


def by_offset(refs, order):
    return [refs[order.index(o)] for o in range(len(order))]


def total_of(refs, rows):
    level = [ref[pl.ds(0, rows), :] for ref in refs]
    while len(level) > 1:
        level = [level[i] + level[i + 1] for i in range(0, len(level), 2)]
    return level[0]


def z_order(n):
    return [3, 1, 2, 0] if n == 4 else list(range(n))


def col_order(n):
    return [3, 1, 2, 0] if n == 4 else list(range(n))


def note_step(hist_ref, hist_out, index, step):
    hist_out[...] = hist_ref[...]
    hist_out[pl.ds(index, 1), :] = jnp.sum(step * step, axis=0, keepdims=True)


def update_dual(iteration, total, dual_ref, hist_ref, dual_out, hist_out):
    dual = dual_ref[...]
    dual_next = jnp.maximum(dual - STEP_DUAL * total, 0.0)
    dual_out[...] = dual_next
    note_step(hist_ref, hist_out, iteration - 1, dual_next - dual)
    return dual_next


def dual_body(iteration, n_msgs, slots, *refs):
    msgs = by_offset(refs[:n_msgs], col_order(n_msgs))
    (dual_ref, hist_ref, cost_ref, one_ref, extra_ref, *blk_refs) = refs[n_msgs : n_msgs + 7]
    (out_ref, dual_out, hist_out, prod_ref) = refs[n_msgs + 7 :]
    rows, _ = dual_out.shape
    blocks = cost_ref.shape[0]

    @pl.when(is_dual_core())
    def _():
        if iteration == 0:
            each = rows // (2 * n_msgs)
            me = lax.axis_index("col")
            for slab in range(2):
                parts = [m[pl.ds(slab * each, each), :] for m in msgs]
                assemble(dual_out, parts, slab * (rows // 2), each, each, me)
            dual_next = dual_out[...]
            hist_out[...] = jnp.zeros_like(hist_out)
            out_ref[pl.ds(blocks, extra_ref.shape[0]), :] = extra_ref[...]
        else:
            dual_next = update_dual(
                iteration, total_of(msgs, rows), dual_ref, hist_ref, dual_out, hist_out
            )
        half = dual_next.astype(BF16)
        slab_rows = rows // 2
        for r in range(rows):
            for s in range(slots):
                at = (r // slab_rows * slots + s) * slab_rows + r % slab_rows
                prod_ref[pl.ds(at, 1), :] = jnp.dot(
                    half[r : r + 1], blk_refs[r // slab_rows][r % slab_rows * slots + s], preferred_element_type=F32
                )
        prod = prod_ref[...]
        high = prod.astype(BF16)
        rest = prod - high.astype(F32)
        mid = rest.astype(BF16)
        low = (rest - mid.astype(F32)).astype(BF16)
        stacked = jnp.concatenate([high, mid, low], axis=0)
        grad = jnp.dot(one_ref[...], stacked, preferred_element_type=F32)
        out_ref[pl.ds(0, blocks), :] = grad - cost_ref[...]


def take(array, index, count, first, rows, stride):
    piece = array[first : first + rows]
    for j in range(1, count):
        at = first + j * stride
        piece = jnp.where(index == j, array[at : at + rows], piece)
    return piece


def last_body(iterations, n_msgs, d_rows, p_rows, *refs):
    msgs = by_offset(refs[:n_msgs], col_order(n_msgs))
    (dual_ref, hist_ref, primal_ref) = refs[n_msgs : n_msgs + 3]
    (out_ref, dual_out, away_ref, next_ref) = refs[n_msgs + 3 :]
    half = next_ref.shape[0] // 2
    dual_core = is_dual_core()

    @pl.when(dual_core)
    def _():
        rows, kept = next_ref.shape[0], hist_ref.shape[0]
        total = total_of(msgs, rows + kept)
        out_ref[pl.ds(0, kept), :] = total[rows:]
        hist_out = out_ref.at[pl.ds(kept, kept)]
        dual_next = update_dual(iterations, total[:rows], dual_ref, hist_ref, next_ref, hist_out)
        col = lax.axis_index("col")
        dual_out[...] = take(dual_next, col, n_msgs, 0, d_rows, d_rows)
        away_ref[pl.ds(0, d_rows), :] = take(dual_next, col, n_msgs, half, d_rows, d_rows)

    @pl.when(jnp.logical_not(dual_core))
    def _():
        away_ref[pl.ds(0, p_rows), :] = primal_ref[pl.ds(DUAL * p_rows, p_rows), :]


def norm_body(n_msgs, p_total, d_total, *refs):
    msgs = by_offset(refs[:n_msgs], z_order(n_msgs))
    norm_out = refs[n_msgs]
    kept = norm_out.shape[1]

    @pl.when(jnp.logical_not(is_dual_core()))
    def _():
        def norms(squares, total):
            column = jnp.sqrt(jnp.sum(squares, axis=1, keepdims=True) / total)
            wide = jnp.broadcast_to(column, (kept, 128))
            row = lax.broadcasted_iota(jnp.int32, wide.shape, 0)
            lane = lax.broadcasted_iota(jnp.int32, wide.shape, 1)
            return jnp.sum(jnp.where(row == lane, wide, 0.0), axis=0, keepdims=True)[:, :kept]

        total = total_of(msgs, 2 * kept)
        norm_out[...] = jnp.concatenate(
            [norms(msgs[0][pl.ds(0, kept), :], p_total), norms(total[kept:], d_total)], axis=0
        )


def finish_body(dual_ref, primal_ref, back_ref, own_ref, got_ref, primal_out, dual_out, norm_out):
    width = dual_ref.shape[1]
    d_rows, p_rows = dual_out.shape[0] // width, primal_out.shape[0] // width
    dual_core = is_dual_core()

    def give(out_ref, rows):
        for r in range(rows.shape[0]):
            out_ref[pl.ds(r * width, width)] = rows[r]

    @pl.when(dual_core)
    def _():
        give(dual_out, dual_ref[...])
        give(primal_out, back_ref[pl.ds(0, p_rows), :])
        norm_out[...] = got_ref[...]

    @pl.when(jnp.logical_not(dual_core))
    def _():
        give(dual_out, back_ref[pl.ds(0, d_rows), :])
        give(primal_out, primal_ref[pl.ds((1 - DUAL) * p_rows, p_rows), :])
        norm_out[...] = own_ref[...]


def pack_body(n, *refs):
    (sources, out_ref, held, sem) = (refs[:n], refs[n], refs[n + 1 : 2 * n + 1], refs[2 * n + 1])
    copies = [
        pltpu.make_async_copy(source, ref, sem.at[i])
        for i, (source, ref) in enumerate(zip(sources, held, strict=True))
    ]
    for copy in copies:
        copy.start()
    for copy in copies:
        copy.wait()
    (cols_ref, *vectors) = held
    width = out_ref.shape[1]
    at = 0
    for ref in vectors:
        for i in range(ref.shape[0] // width):
            out_ref[at, :] = ref[pl.ds(i * width, width)]
            at += 1
    out_ref[pl.ds(at, cols_ref.shape[0]), pl.ds(0, cols_ref.shape[1])] = cols_ref[...].astype(F32)


def pack_call(out, *arrays):
    n = len(arrays)
    return pl.pallas_call(
        functools.partial(pack_body, n),
        out_shape=out,
        in_specs=[pl.BlockSpec(memory_space=pltpu.HBM)] * n,
        out_specs=pl.BlockSpec(memory_space=pltpu.VMEM),
        scratch_shapes=[pltpu.VMEM(a.shape, a.dtype) for a in arrays]
        + [pltpu.SemaphoreType.DMA((n,))],
        compiler_params=pltpu.CompilerParams(vmem_limit_bytes=66985984),
    )(*arrays)


def setup_body(d_rows, p_rows, slab_rows, slots, n_z, n_col, *refs):
    (own_ref, other_ref, dual_out, extra_out, cost_out, right_out, one_out, pick_out) = refs[:8]
    column_ref = refs[8]
    dual_core = is_dual_core()
    first = jnp.where(dual_core, own_ref[...], other_ref[...])
    second = jnp.where(dual_core, other_ref[...], own_ref[...])
    z, col = lax.axis_index("row") // 2, lax.axis_index("col")
    at = 0
    for slab, part in enumerate((first, second)):
        dual_out[pl.ds(slab * d_rows, d_rows), :] = part[:d_rows]
    at += d_rows
    for slab, part in enumerate((first, second)):
        piece = part[at : at + d_rows]
        for j in range(n_col):
            right_out[pl.ds(slab * slab_rows + j * d_rows, d_rows), :] = jnp.where(
                col == j, piece, 0.0
            )
    at += d_rows
    for slab, part in enumerate((first, second)):
        piece = part[at : at + p_rows]
        for j in range(n_z):
            cost_out[pl.ds((2 * j + slab ^ DUAL) * p_rows, p_rows), :] = jnp.where(
                z == j, piece, 0.0
            )
    at += p_rows
    for k in range(3):
        for slab, part in enumerate((first, second)):
            extra_out[pl.ds((2 * k + slab ^ DUAL) * p_rows, p_rows), :] = part[at : at + p_rows]
        at += p_rows
    entries, blocks = pick_out.shape
    side, lanes = -(-blocks // 128) * 128, column_ref.shape[1]
    column_ref[...] = jnp.full(column_ref.shape, -1.0, F32)
    for k, (part, slot) in enumerate((p, s) for p in (first, second) for s in range(slots)):
        column_ref[pl.ds(0, 1), pl.ds(k * slab_rows, slab_rows)] = part[
            at + slot : at + slot + 1, :slab_rows
        ]
    iota = lax.broadcasted_iota(jnp.int32, (side, lanes), 0).astype(F32)
    column = jnp.broadcast_to(column_ref[pl.ds(0, 1), :], (side, lanes))
    hot = jnp.where(column == iota, 1.0, 0.0)
    pick_out[...] = hot.T[:entries, :blocks].astype(BF16)
    one = hot[:blocks, :entries]
    one_out[...] = jnp.concatenate([one] * 3, axis=1).astype(BF16)


def primal_body(iteration, last, n_msgs, slots, *refs):
    msgs = by_offset(refs[:n_msgs], z_order(n_msgs))
    (primal_ref, low_ref, up_ref, hist_ref, right_ref, pick_ref, *blk_refs) = refs[
        n_msgs : n_msgs + 8
    ]
    (out_ref, primal_out, *rest) = refs[n_msgs + 8 :]
    blk_refs = blk_refs[::-1]
    blocks = primal_ref.shape[0]
    rows = right_ref.shape[0]
    slab_rows = rows // 2
    hist_out = out_ref.at[pl.ds(rows, hist_ref.shape[0])] if last else rest[0]
    bounds_out = rest[1:]

    @pl.when(jnp.logical_not(is_dual_core()))
    def _():
        total = total_of(msgs, blocks)
        if iteration == 0:
            each = blocks // n_msgs
            me = lax.axis_index("row") // 2
            for k, ref in enumerate((primal_out, *bounds_out)):
                parts = [m[pl.ds(blocks + k * each, each), :] for m in msgs]
                assemble(ref, parts, 0, each, each, me)
            primal, low, up = primal_out[...], bounds_out[0][...], bounds_out[1][...]
            hist_out[...] = jnp.zeros_like(hist_out)
        else:
            primal, low, up = primal_ref[...], low_ref[...], up_ref[...]
        primal_next = jnp.minimum(up, jnp.maximum(low, primal + STEP_PRIMAL * total))
        if last:
            index = lax.axis_index("row") // 2
            each = primal_out.shape[0]
            primal_out[...] = take(primal_next, index, n_msgs, 0, each, each)
        else:
            primal_out[...] = primal_next
        note_step(hist_out if iteration == 0 else hist_ref, hist_out, iteration, primal_next - primal)
        ext = (2.0 * primal_next - primal).astype(BF16)
        picked = jnp.dot(pick_ref[...], ext, preferred_element_type=F32).astype(BF16)
        for r in range(rows):
            acc = -right_ref[pl.ds(r, 1), :]
            for s in range(slots):
                at = (r // slab_rows * slots + s) * slab_rows + r % slab_rows
                acc = acc + jnp.dot(
                    picked[at : at + 1],
                    blk_refs[r // slab_rows][r % slab_rows * slots + s],
                    preferred_element_type=F32,
                )
            out_ref[pl.ds(r, 1), :] = acc


def weights_body(in_ref, out_ref, sem):
    copy = pltpu.make_async_copy(in_ref, out_ref, sem)
    copy.start()
    copy.wait()

    @pl.when(jnp.logical_not(is_dual_core()))
    def _():
        def step(i, carry):
            for k in range(8):
                out_ref[i * 8 + k] = out_ref[i * 8 + k].T
            return carry

        lax.fori_loop(0, in_ref.shape[0] // 8, step, 0)


def weights_call(blocks):
    return pl.pallas_call(
        weights_body,
        out_shape=jax.ShapeDtypeStruct(blocks.shape, BF16),
        in_specs=[pl.BlockSpec(memory_space=pltpu.HBM)],
        out_specs=pl.BlockSpec(memory_space=pltpu.VMEM),
        scratch_shapes=[pltpu.SemaphoreType.DMA],
        compiler_params=pltpu.CompilerParams(vmem_limit_bytes=8 * 2**20),
    )(blocks)


def local_call(body, outs, scratch, n_in):
    return pl.pallas_call(
        body,
        out_shape=outs,
        in_specs=[pl.BlockSpec(memory_space=pltpu.VMEM)] * n_in,
        out_specs=[pl.BlockSpec(memory_space=pltpu.VMEM)] * len(outs),
        scratch_shapes=scratch,
        compiler_params=pltpu.CompilerParams(vmem_limit_bytes=4 * 2**20),
    )


def per_device(
    blocks, block_cols, objective, lower_bound, upper_bound, right_side, primal_init, dual_init
):
    slab_rows, slots, width = blocks.shape[0], blocks.shape[1], blocks.shape[2]
    n_row, n_col = lax.axis_size("row"), lax.axis_size("col")
    n_z = n_row // 2
    p_rows = primal_init.shape[0] // width
    d_rows = dual_init.shape[0] // width
    col_blocks = p_rows * n_row
    rows = 2 * slab_rows
    entries = rows * slots

    swap_pairs = [(r, r ^ 1) for r in range(n_row)]

    def over_z(src, o):
        away = [(2 * k + src, 2 * (k ^ o) + 1 - src) for k in range(n_z)]
        return away + [(2 * k + 1 - src, 2 * k + src) for k in range(n_z)]

    def over_col(src, o):
        pairs = []
        for k in range(n_z):
            for c in range(n_col):
                pairs.append(((2 * k + src) * n_col + c, (2 * k + 1 - src) * n_col + (c ^ o)))
                pairs.append(((2 * k + 1 - src) * n_col + c, (2 * k + src) * n_col + c))
        return pairs

    def to_primal(x):
        return [lax.ppermute(x, "row", over_z(DUAL, o)) for o in z_order(n_z)]

    def to_dual(x):
        return [lax.ppermute(x, ("row", "col"), over_col(1 - DUAL, o)) for o in col_order(n_col)]

    def shape(n, wide=width, dtype=F32):
        return jax.ShapeDtypeStruct((n, wide), dtype)

    mine = blocks.reshape(slab_rows * slots, width, width)
    own = pack_call(
        shape(2 * d_rows + 4 * p_rows + slots),
        block_cols.T, dual_init, right_side, objective, primal_init, lower_bound, upper_bound,
    )
    gated, own = lax.optimization_barrier((mine, own))
    other = lax.ppermute(own, "row", swap_pairs)
    theirs = lax.ppermute(gated, "row", swap_pairs)
    dual_part, extra, cost, right, one_three, pick = local_call(
        functools.partial(setup_body, d_rows, p_rows, slab_rows, slots, n_z, n_col),
        [
            shape(2 * d_rows),
            shape(6 * p_rows),
            shape(col_blocks),
            shape(rows),
            shape(col_blocks, 3 * entries, BF16),
            shape(entries, col_blocks, BF16),
        ],
        [pltpu.VMEM((8, -(-entries // 128) * 128), F32)],
        2,
    )(own, other)
    own_weights = weights_call(mine)
    dual_part, own_weights = lax.optimization_barrier((dual_part, own_weights))
    weights = (own_weights, weights_call(theirs))

    hist_rows = -(-ITERS // 8) * 8
    dual = right
    primal = cost
    bounds = (cost, cost)
    primal_hist = dual_hist = jnp.zeros((hist_rows, width), F32)
    products = pltpu.VMEM((entries, width), F32)

    arrived = to_dual(dual_part)
    for iteration in range(ITERS):
        first, last = iteration == 0, iteration == ITERS - 1
        message, dual, dual_hist = local_call(
            functools.partial(dual_body, iteration, n_col, slots),
            [shape(col_blocks + (6 * p_rows if first else 0)), shape(rows), shape(hist_rows)],
            [products],
            n_col + 7,
        )(*arrived, dual, dual_hist, cost, one_three, extra, *weights)
        arrived = to_primal(message)
        message, primal, *others = local_call(
            functools.partial(primal_body, iteration, last, n_z, slots),
            [
                shape(rows + (hist_rows if last else 0)),
                shape(2 * p_rows if last else col_blocks),
            ]
            + [shape(hist_rows)] * (not last)
            + [shape(col_blocks)] * (2 if first else 0),
            [],
            n_z + 8,
        )(*arrived, primal, *bounds, primal_hist, right, pick, *weights)
        if first:
            bounds = others[1:]
        if not last:
            primal_hist = others[0]
        arrived = to_dual(message)
    message, dual, away = local_call(
        functools.partial(last_body, ITERS, n_col, d_rows, p_rows),
        [shape(2 * hist_rows), shape(d_rows), shape(max(p_rows, d_rows))],
        [pltpu.VMEM((rows, width), F32)],
        n_col + 3,
    )(*arrived, dual, dual_hist, primal)
    back = lax.ppermute(away, "row", swap_pairs)
    arrived = to_primal(message)
    (norms,) = local_call(
        functools.partial(
            norm_body,
            n_z,
            float(primal_init.shape[0] * n_row * n_col),
            float(dual_init.shape[0] * n_row * n_col),
        ),
        [shape(2, hist_rows)],
        [],
        n_z,
    )(*arrived)
    primal_out, dual_out, norms = local_call(
        finish_body,
        [
            jax.ShapeDtypeStruct(primal_init.shape, F32),
            jax.ShapeDtypeStruct(dual_init.shape, F32),
            shape(2, hist_rows),
        ],
        [],
        5,
    )(dual, primal, back, norms, lax.ppermute(norms, "row", swap_pairs))
    return (primal_out, dual_out, norms.T[:ITERS])


def solution(mesh):
    in_specs = (
        P("row", "col", None, None),
        P("row", "col"),
        P(("col", "row")),
        P(("col", "row")),
        P(("col", "row")),
        P(("row", "col")),
        P(("col", "row")),
        P(("row", "col")),
    )
    out_specs = (P(("col", "row")), P(("row", "col")), P())
    return jax.shard_map(
        per_device, mesh=mesh, in_specs=in_specs, out_specs=out_specs, check_vma=False
    )
```

```python
import functools

import jax
import jax.numpy as jnp
from jax import lax
from jax.experimental import pallas as pl
from jax.experimental.pallas import tpu as pltpu
from jax.sharding import PartitionSpec as P


ITERS = 8
STEP_PRIMAL = 0.5
STEP_DUAL = 0.5

VECTOR_ROWS = 7
DUAL = 0

F32 = jnp.float32
BF16 = jnp.bfloat16


def is_dual_core():
    return lax.axis_index("row") % 2 == DUAL


def assemble(ref, parts, first, rows, stride, me):
    for j in range(len(parts)):
        piece = parts[0]
        for o in range(1, len(parts)):
            piece = jnp.where(me == (j ^ o), parts[o], piece)
        ref[pl.ds(first + j * stride, rows), :] = piece


def by_offset(refs, order):
    return [refs[order.index(o)] for o in range(len(order))]


def total_of(refs, rows):
    level = [ref[pl.ds(0, rows), :] for ref in refs]
    while len(level) > 1:
        level = [level[i] + level[i + 1] for i in range(0, len(level), 2)]
    return level[0]


def vector_rows(rows):
    step = rows // VECTOR_ROWS if VECTOR_ROWS else rows
    return [step // 2 + i * step for i in range(VECTOR_ROWS)]


def weigh(pairs):
    chunk = 16
    total = None
    for i in range(0, pairs[0][0].shape[0], chunk):
        for block, column in pairs:
            term = block[i : i + chunk].astype(F32) * column[i : i + chunk]
            total = term if total is None else total + term
    return jnp.sum(total, axis=0, keepdims=True)


def z_order(n):
    return [3, 1, 2, 0] if n == 4 else list(range(n))


def col_order(n):
    return [3, 1, 2, 0] if n == 4 else list(range(n))


def note_step(hist_ref, hist_out, index, step):
    hist_out[...] = hist_ref[...]
    hist_out[pl.ds(index, 1), :] = jnp.sum(step * step, axis=0, keepdims=True)


def update_dual(iteration, total, dual_ref, hist_ref, dual_out, hist_out):
    dual = dual_ref[...]
    dual_next = jnp.maximum(dual - STEP_DUAL * total, 0.0)
    dual_out[...] = dual_next
    note_step(hist_ref, hist_out, iteration - 1, dual_next - dual)
    return dual_next


def dual_body(iteration, n_msgs, slots, *refs):
    msgs = by_offset(refs[:n_msgs], col_order(n_msgs))
    (dual_ref, hist_ref, cost_ref, one_ref, extra_ref, *blk_refs) = refs[n_msgs : n_msgs + 7]
    (out_ref, dual_out, hist_out, prod_ref) = refs[n_msgs + 7 :]
    rows, _ = dual_out.shape
    blocks = cost_ref.shape[0]

    @pl.when(is_dual_core())
    def _():
        if iteration == 0:
            each = rows // (2 * n_msgs)
            me = lax.axis_index("col")
            for slab in range(2):
                parts = [m[pl.ds(slab * each, each), :] for m in msgs]
                assemble(dual_out, parts, slab * (rows // 2), each, each, me)
            dual_next = dual_out[...]
            hist_out[...] = jnp.zeros_like(hist_out)
            out_ref[pl.ds(blocks, extra_ref.shape[0]), :] = extra_ref[...]
        else:
            dual_next = update_dual(
                iteration, total_of(msgs, rows), dual_ref, hist_ref, dual_out, hist_out
            )
        half = dual_next.astype(BF16)
        slab_rows = rows // 2
        by_vector = vector_rows(rows)
        turned = half[: 8 * (max(by_vector) // 8 + 1)].astype(F32).T if by_vector else None
        for r in range(rows):
            for s in range(slots):
                at = (r // slab_rows * slots + s) * slab_rows + r % slab_rows
                block = blk_refs[r // slab_rows][r % slab_rows * slots + s]
                if r in by_vector:
                    prod_ref[pl.ds(at, 1), :] = weigh(((block, turned[:, r : r + 1]),))
                else:
                    prod_ref[pl.ds(at, 1), :] = jnp.dot(
                        half[r : r + 1], block, preferred_element_type=F32
                    )
        prod = prod_ref[...]
        high = prod.astype(BF16)
        rest = prod - high.astype(F32)
        mid = rest.astype(BF16)
        low = (rest - mid.astype(F32)).astype(BF16)
        stacked = jnp.concatenate([high, mid, low], axis=0)
        grad = jnp.dot(one_ref[...], stacked, preferred_element_type=F32)
        out_ref[pl.ds(0, blocks), :] = grad - cost_ref[...]


def take(array, index, count, first, rows, stride):
    piece = array[first : first + rows]
    for j in range(1, count):
        at = first + j * stride
        piece = jnp.where(index == j, array[at : at + rows], piece)
    return piece


def last_body(iterations, n_msgs, d_rows, p_rows, *refs):
    msgs = by_offset(refs[:n_msgs], col_order(n_msgs))
    (dual_ref, hist_ref, primal_ref) = refs[n_msgs : n_msgs + 3]
    (out_ref, dual_out, away_ref, next_ref) = refs[n_msgs + 3 :]
    half = next_ref.shape[0] // 2
    dual_core = is_dual_core()

    @pl.when(dual_core)
    def _():
        rows, kept = next_ref.shape[0], hist_ref.shape[0]
        total = total_of(msgs, rows + kept)
        out_ref[pl.ds(0, kept), :] = total[rows:]
        hist_out = out_ref.at[pl.ds(kept, kept)]
        dual_next = update_dual(iterations, total[:rows], dual_ref, hist_ref, next_ref, hist_out)
        col = lax.axis_index("col")
        dual_out[...] = take(dual_next, col, n_msgs, 0, d_rows, d_rows)
        away_ref[pl.ds(0, d_rows), :] = take(dual_next, col, n_msgs, half, d_rows, d_rows)

    @pl.when(jnp.logical_not(dual_core))
    def _():
        away_ref[pl.ds(0, p_rows), :] = primal_ref[pl.ds(DUAL * p_rows, p_rows), :]


def norm_body(n_msgs, p_total, d_total, *refs):
    msgs = by_offset(refs[:n_msgs], z_order(n_msgs))
    norm_out = refs[n_msgs]
    kept = norm_out.shape[1]

    @pl.when(jnp.logical_not(is_dual_core()))
    def _():
        def norms(squares, total):
            column = jnp.sqrt(jnp.sum(squares, axis=1, keepdims=True) / total)
            wide = jnp.broadcast_to(column, (kept, 128))
            row = lax.broadcasted_iota(jnp.int32, wide.shape, 0)
            lane = lax.broadcasted_iota(jnp.int32, wide.shape, 1)
            return jnp.sum(jnp.where(row == lane, wide, 0.0), axis=0, keepdims=True)[:, :kept]

        total = total_of(msgs, 2 * kept)
        norm_out[...] = jnp.concatenate(
            [norms(msgs[0][pl.ds(0, kept), :], p_total), norms(total[kept:], d_total)], axis=0
        )


def finish_body(dual_ref, primal_ref, back_ref, own_ref, got_ref, primal_out, dual_out, norm_out):
    width = dual_ref.shape[1]
    d_rows, p_rows = dual_out.shape[0] // width, primal_out.shape[0] // width
    dual_core = is_dual_core()

    def give(out_ref, rows):
        for r in range(rows.shape[0]):
            out_ref[pl.ds(r * width, width)] = rows[r]

    @pl.when(dual_core)
    def _():
        give(dual_out, dual_ref[...])
        give(primal_out, back_ref[pl.ds(0, p_rows), :])
        norm_out[...] = got_ref[...]

    @pl.when(jnp.logical_not(dual_core))
    def _():
        give(dual_out, back_ref[pl.ds(0, d_rows), :])
        give(primal_out, primal_ref[pl.ds((1 - DUAL) * p_rows, p_rows), :])
        norm_out[...] = own_ref[...]


def pack_body(n, *refs):
    (sources, out_ref, held, sem) = (refs[:n], refs[n], refs[n + 1 : 2 * n + 1], refs[2 * n + 1])
    copies = [
        pltpu.make_async_copy(source, ref, sem.at[i])
        for i, (source, ref) in enumerate(zip(sources, held, strict=True))
    ]
    for copy in copies:
        copy.start()
    for copy in copies:
        copy.wait()
    (cols_ref, *vectors) = held
    width = out_ref.shape[1]
    at = 0
    for ref in vectors:
        for i in range(ref.shape[0] // width):
            out_ref[at, :] = ref[pl.ds(i * width, width)]
            at += 1
    out_ref[pl.ds(at, cols_ref.shape[0]), pl.ds(0, cols_ref.shape[1])] = cols_ref[...].astype(F32)


def pack_call(out, *arrays):
    n = len(arrays)
    return pl.pallas_call(
        functools.partial(pack_body, n),
        out_shape=out,
        in_specs=[pl.BlockSpec(memory_space=pltpu.HBM)] * n,
        out_specs=pl.BlockSpec(memory_space=pltpu.VMEM),
        scratch_shapes=[pltpu.VMEM(a.shape, a.dtype) for a in arrays]
        + [pltpu.SemaphoreType.DMA((n,))],
        compiler_params=pltpu.CompilerParams(vmem_limit_bytes=66985984),
    )(*arrays)


def setup_body(d_rows, p_rows, slab_rows, slots, n_z, n_col, *refs):
    (own_ref, other_ref, dual_out, extra_out, cost_out, right_out, one_out, pick_out) = refs[:8]
    column_ref = refs[8]
    dual_core = is_dual_core()
    first = jnp.where(dual_core, own_ref[...], other_ref[...])
    second = jnp.where(dual_core, other_ref[...], own_ref[...])
    z, col = lax.axis_index("row") // 2, lax.axis_index("col")
    at = 0
    for slab, part in enumerate((first, second)):
        dual_out[pl.ds(slab * d_rows, d_rows), :] = part[:d_rows]
    at += d_rows
    for slab, part in enumerate((first, second)):
        piece = part[at : at + d_rows]
        for j in range(n_col):
            right_out[pl.ds(slab * slab_rows + j * d_rows, d_rows), :] = jnp.where(
                col == j, piece, 0.0
            )
    at += d_rows
    for slab, part in enumerate((first, second)):
        piece = part[at : at + p_rows]
        for j in range(n_z):
            cost_out[pl.ds((2 * j + slab ^ DUAL) * p_rows, p_rows), :] = jnp.where(
                z == j, piece, 0.0
            )
    at += p_rows
    for k in range(3):
        for slab, part in enumerate((first, second)):
            extra_out[pl.ds((2 * k + slab ^ DUAL) * p_rows, p_rows), :] = part[at : at + p_rows]
        at += p_rows
    entries, blocks = pick_out.shape
    side, lanes = -(-blocks // 128) * 128, column_ref.shape[1]
    column_ref[...] = jnp.full(column_ref.shape, -1.0, F32)
    for k, (part, slot) in enumerate((p, s) for p in (first, second) for s in range(slots)):
        column_ref[pl.ds(0, 1), pl.ds(k * slab_rows, slab_rows)] = part[
            at + slot : at + slot + 1, :slab_rows
        ]
    iota = lax.broadcasted_iota(jnp.int32, (side, lanes), 0).astype(F32)
    column = jnp.broadcast_to(column_ref[pl.ds(0, 1), :], (side, lanes))
    hot = jnp.where(column == iota, 1.0, 0.0)
    pick_out[...] = hot.T[:entries, :blocks].astype(BF16)
    one = hot[:blocks, :entries]
    one_out[...] = jnp.concatenate([one] * 3, axis=1).astype(BF16)


def primal_body(iteration, last, n_msgs, slots, *refs):
    msgs = by_offset(refs[:n_msgs], z_order(n_msgs))
    (primal_ref, low_ref, up_ref, hist_ref, right_ref, pick_ref, *blk_refs) = refs[
        n_msgs : n_msgs + 8
    ]
    (out_ref, primal_out, *rest) = refs[n_msgs + 8 :]
    blk_refs = blk_refs[::-1]
    blocks = primal_ref.shape[0]
    rows = right_ref.shape[0]
    slab_rows = rows // 2
    hist_out = out_ref.at[pl.ds(rows, hist_ref.shape[0])] if last else rest[0]
    bounds_out = rest[1:]

    @pl.when(jnp.logical_not(is_dual_core()))
    def _():
        total = total_of(msgs, blocks)
        if iteration == 0:
            each = blocks // n_msgs
            me = lax.axis_index("row") // 2
            for k, ref in enumerate((primal_out, *bounds_out)):
                parts = [m[pl.ds(blocks + k * each, each), :] for m in msgs]
                assemble(ref, parts, 0, each, each, me)
            primal, low, up = primal_out[...], bounds_out[0][...], bounds_out[1][...]
            hist_out[...] = jnp.zeros_like(hist_out)
        else:
            primal, low, up = primal_ref[...], low_ref[...], up_ref[...]
        primal_next = jnp.minimum(up, jnp.maximum(low, primal + STEP_PRIMAL * total))
        if last:
            index = lax.axis_index("row") // 2
            each = primal_out.shape[0]
            primal_out[...] = take(primal_next, index, n_msgs, 0, each, each)
        else:
            primal_out[...] = primal_next
        note_step(hist_out if iteration == 0 else hist_ref, hist_out, iteration, primal_next - primal)
        ext = (2.0 * primal_next - primal).astype(BF16)
        found = jnp.dot(pick_ref[...], ext, preferred_element_type=F32)
        picked = found.astype(BF16)
        by_vector = vector_rows(rows)
        turned = found.T if by_vector else None
        for r in range(rows):
            acc = -right_ref[pl.ds(r, 1), :]
            pairs = []
            for s in range(slots):
                at = (r // slab_rows * slots + s) * slab_rows + r % slab_rows
                block = blk_refs[r // slab_rows][r % slab_rows * slots + s]
                if r in by_vector:
                    pairs.append((block, turned[:, at : at + 1]))
                else:
                    acc = acc + jnp.dot(picked[at : at + 1], block, preferred_element_type=F32)
            if pairs:
                acc = acc + weigh(pairs)
            out_ref[pl.ds(r, 1), :] = acc


def weights_body(in_ref, out_ref, sem):
    copy = pltpu.make_async_copy(in_ref, out_ref, sem)
    copy.start()
    copy.wait()

    @pl.when(jnp.logical_not(is_dual_core()))
    def _():
        def step(i, carry):
            for k in range(8):
                out_ref[i * 8 + k] = out_ref[i * 8 + k].T
            return carry

        lax.fori_loop(0, in_ref.shape[0] // 8, step, 0)


def weights_call(blocks):
    return pl.pallas_call(
        weights_body,
        out_shape=jax.ShapeDtypeStruct(blocks.shape, BF16),
        in_specs=[pl.BlockSpec(memory_space=pltpu.HBM)],
        out_specs=pl.BlockSpec(memory_space=pltpu.VMEM),
        scratch_shapes=[pltpu.SemaphoreType.DMA],
        compiler_params=pltpu.CompilerParams(vmem_limit_bytes=8 * 2**20),
    )(blocks)


def local_call(body, outs, scratch, n_in):
    return pl.pallas_call(
        body,
        out_shape=outs,
        in_specs=[pl.BlockSpec(memory_space=pltpu.VMEM)] * n_in,
        out_specs=[pl.BlockSpec(memory_space=pltpu.VMEM)] * len(outs),
        scratch_shapes=scratch,
        compiler_params=pltpu.CompilerParams(vmem_limit_bytes=4 * 2**20),
    )


def per_device(
    blocks, block_cols, objective, lower_bound, upper_bound, right_side, primal_init, dual_init
):
    slab_rows, slots, width = blocks.shape[0], blocks.shape[1], blocks.shape[2]
    n_row, n_col = lax.axis_size("row"), lax.axis_size("col")
    n_z = n_row // 2
    p_rows = primal_init.shape[0] // width
    d_rows = dual_init.shape[0] // width
    col_blocks = p_rows * n_row
    rows = 2 * slab_rows
    entries = rows * slots

    swap_pairs = [(r, r ^ 1) for r in range(n_row)]

    def over_z(src, o):
        away = [(2 * k + src, 2 * (k ^ o) + 1 - src) for k in range(n_z)]
        return away + [(2 * k + 1 - src, 2 * k + src) for k in range(n_z)]

    def over_col(src, o):
        pairs = []
        for k in range(n_z):
            for c in range(n_col):
                pairs.append(((2 * k + src) * n_col + c, (2 * k + 1 - src) * n_col + (c ^ o)))
                pairs.append(((2 * k + 1 - src) * n_col + c, (2 * k + src) * n_col + c))
        return pairs

    def to_primal(x):
        return [lax.ppermute(x, "row", over_z(DUAL, o)) for o in z_order(n_z)]

    def to_dual(x):
        return [lax.ppermute(x, ("row", "col"), over_col(1 - DUAL, o)) for o in col_order(n_col)]

    def shape(n, wide=width, dtype=F32):
        return jax.ShapeDtypeStruct((n, wide), dtype)

    mine = blocks.reshape(slab_rows * slots, width, width)
    own = pack_call(
        shape(2 * d_rows + 4 * p_rows + slots),
        block_cols.T, dual_init, right_side, objective, primal_init, lower_bound, upper_bound,
    )
    gated, own = lax.optimization_barrier((mine, own))
    other = lax.ppermute(own, "row", swap_pairs)
    theirs = lax.ppermute(gated, "row", swap_pairs)
    dual_part, extra, cost, right, one_three, pick = local_call(
        functools.partial(setup_body, d_rows, p_rows, slab_rows, slots, n_z, n_col),
        [
            shape(2 * d_rows),
            shape(6 * p_rows),
            shape(col_blocks),
            shape(rows),
            shape(col_blocks, 3 * entries, BF16),
            shape(entries, col_blocks, BF16),
        ],
        [pltpu.VMEM((8, -(-entries // 128) * 128), F32)],
        2,
    )(own, other)
    own_weights = weights_call(mine)
    dual_part, own_weights = lax.optimization_barrier((dual_part, own_weights))
    weights = (own_weights, weights_call(theirs))

    hist_rows = -(-ITERS // 8) * 8
    dual = right
    primal = cost
    bounds = (cost, cost)
    primal_hist = dual_hist = jnp.zeros((hist_rows, width), F32)
    products = pltpu.VMEM((entries, width), F32)

    arrived = to_dual(dual_part)
    for iteration in range(ITERS):
        first, last = iteration == 0, iteration == ITERS - 1
        message, dual, dual_hist = local_call(
            functools.partial(dual_body, iteration, n_col, slots),
            [shape(col_blocks + (6 * p_rows if first else 0)), shape(rows), shape(hist_rows)],
            [products],
            n_col + 7,
        )(*arrived, dual, dual_hist, cost, one_three, extra, *weights)
        arrived = to_primal(message)
        message, primal, *others = local_call(
            functools.partial(primal_body, iteration, last, n_z, slots),
            [
                shape(rows + (hist_rows if last else 0)),
                shape(2 * p_rows if last else col_blocks),
            ]
            + [shape(hist_rows)] * (not last)
            + [shape(col_blocks)] * (2 if first else 0),
            [],
            n_z + 8,
        )(*arrived, primal, *bounds, primal_hist, right, pick, *weights)
        if first:
            bounds = others[1:]
        if not last:
            primal_hist = others[0]
        arrived = to_dual(message)
    message, dual, away = local_call(
        functools.partial(last_body, ITERS, n_col, d_rows, p_rows),
        [shape(2 * hist_rows), shape(d_rows), shape(max(p_rows, d_rows))],
        [pltpu.VMEM((rows, width), F32)],
        n_col + 3,
    )(*arrived, dual, dual_hist, primal)
    back = lax.ppermute(away, "row", swap_pairs)
    arrived = to_primal(message)
    (norms,) = local_call(
        functools.partial(
            norm_body,
            n_z,
            float(primal_init.shape[0] * n_row * n_col),
            float(dual_init.shape[0] * n_row * n_col),
        ),
        [shape(2, hist_rows)],
        [],
        n_z,
    )(*arrived)
    primal_out, dual_out, norms = local_call(
        finish_body,
        [
            jax.ShapeDtypeStruct(primal_init.shape, F32),
            jax.ShapeDtypeStruct(dual_init.shape, F32),
            shape(2, hist_rows),
        ],
        [],
        5,
    )(dual, primal, back, norms, lax.ppermute(norms, "row", swap_pairs))
    return (primal_out, dual_out, norms.T[:ITERS])


def solution(mesh):
    in_specs = (
        P("row", "col", None, None),
        P("row", "col"),
        P(("col", "row")),
        P(("col", "row")),
        P(("col", "row")),
        P(("row", "col")),
        P(("col", "row")),
        P(("row", "col")),
    )
    out_specs = (P(("col", "row")), P(("row", "col")), P())
    return jax.shard_map(
        per_device, mesh=mesh, in_specs=in_specs, out_specs=out_specs, check_vma=False
    )
```

```python
import functools

import jax
import jax.numpy as jnp
from jax import lax
from jax.experimental import pallas as pl
from jax.experimental.pallas import tpu as pltpu
from jax.sharding import PartitionSpec as P


ITERS = 8
STEP_PRIMAL = 0.5
STEP_DUAL = 0.5

VECTOR_ROWS = 7
DUAL = 0

F32 = jnp.float32
BF16 = jnp.bfloat16


def is_dual_core():
    return lax.axis_index("row") % 2 == DUAL


def assemble(ref, parts, first, rows, stride, me):
    for j in range(len(parts)):
        piece = parts[0]
        for o in range(1, len(parts)):
            piece = jnp.where(me == (j ^ o), parts[o], piece)
        ref[pl.ds(first + j * stride, rows), :] = piece


def by_offset(refs, order):
    return [refs[order.index(o)] for o in range(len(order))]


def total_of(refs, rows):
    level = [ref[pl.ds(0, rows), :] for ref in refs]
    while len(level) > 1:
        level = [level[i] + level[i + 1] for i in range(0, len(level), 2)]
    return level[0]


def vector_rows(rows):
    step = rows // VECTOR_ROWS if VECTOR_ROWS else rows
    return [step // 2 + i * step for i in range(VECTOR_ROWS)]


def weigh(pairs):
    chunk = 16
    total = None
    for i in range(0, pairs[0][0].shape[0], chunk):
        for block, column in pairs:
            term = block[i : i + chunk].astype(F32) * column[i : i + chunk]
            total = term if total is None else total + term
    return jnp.sum(total, axis=0, keepdims=True)


def z_order(n):
    return [3, 1, 2, 0] if n == 4 else list(range(n))


def col_order(n):
    return [3, 1, 2, 0] if n == 4 else list(range(n))


def note_step(hist_ref, hist_out, index, step):
    hist_out[...] = hist_ref[...]
    hist_out[pl.ds(index, 1), :] = jnp.sum(step * step, axis=0, keepdims=True)


def update_dual(iteration, total, dual_ref, hist_ref, dual_out, hist_out):
    dual = dual_ref[...]
    dual_next = jnp.maximum(dual - STEP_DUAL * total, 0.0)
    dual_out[...] = dual_next
    note_step(hist_ref, hist_out, iteration - 1, dual_next - dual)
    return dual_next


def dual_body(iteration, n_msgs, slots, *refs):
    msgs = by_offset(refs[:n_msgs], col_order(n_msgs))
    (dual_ref, hist_ref, cost_ref, one_ref, extra_ref, *blk_refs) = refs[n_msgs : n_msgs + 7]
    (out_ref, dual_out, hist_out, prod_ref) = refs[n_msgs + 7 :]
    rows, _ = dual_out.shape
    blocks = cost_ref.shape[0]

    @pl.when(is_dual_core())
    def _():
        if iteration == 0:
            each = rows // (2 * n_msgs)
            me = lax.axis_index("col")
            for slab in range(2):
                parts = [m[pl.ds(slab * each, each), :] for m in msgs]
                assemble(dual_out, parts, slab * (rows // 2), each, each, me)
            dual_next = dual_out[...]
            hist_out[...] = jnp.zeros_like(hist_out)
            out_ref[pl.ds(blocks, extra_ref.shape[0]), :] = extra_ref[...]
        else:
            dual_next = update_dual(
                iteration, total_of(msgs, rows), dual_ref, hist_ref, dual_out, hist_out
            )
        half = dual_next.astype(BF16)
        slab_rows = rows // 2
        by_vector = vector_rows(rows)
        turned = half[: 8 * (max(by_vector) // 8 + 1)].astype(F32).T if by_vector else None
        for r in range(rows):
            for s in range(slots):
                at = (r // slab_rows * slots + s) * slab_rows + r % slab_rows
                block = blk_refs[r // slab_rows][r % slab_rows * slots + s]
                if r in by_vector:
                    prod_ref[pl.ds(at, 1), :] = weigh(((block, turned[:, r : r + 1]),))
                else:
                    prod_ref[pl.ds(at, 1), :] = jnp.dot(
                        half[r : r + 1], block, preferred_element_type=F32
                    )
        prod = prod_ref[...]
        high = prod.astype(BF16)
        rest = prod - high.astype(F32)
        mid = rest.astype(BF16)
        low = (rest - mid.astype(F32)).astype(BF16)
        stacked = jnp.concatenate([high, mid, low], axis=0)
        grad = jnp.dot(one_ref[...], stacked, preferred_element_type=F32)
        out_ref[pl.ds(0, blocks), :] = grad - cost_ref[...]


def take(array, index, count, first, rows, stride):
    piece = array[first : first + rows]
    for j in range(1, count):
        at = first + j * stride
        piece = jnp.where(index == j, array[at : at + rows], piece)
    return piece


def last_body(iterations, n_msgs, d_rows, p_rows, *refs):
    msgs = by_offset(refs[:n_msgs], col_order(n_msgs))
    (dual_ref, hist_ref, primal_ref) = refs[n_msgs : n_msgs + 3]
    (out_ref, dual_out, away_ref, next_ref) = refs[n_msgs + 3 :]
    half = next_ref.shape[0] // 2
    dual_core = is_dual_core()

    @pl.when(dual_core)
    def _():
        rows, kept = next_ref.shape[0], hist_ref.shape[0]
        total = total_of(msgs, rows + kept)
        out_ref[pl.ds(0, kept), :] = total[rows:]
        hist_out = out_ref.at[pl.ds(kept, kept)]
        dual_next = update_dual(iterations, total[:rows], dual_ref, hist_ref, next_ref, hist_out)
        col = lax.axis_index("col")
        dual_out[...] = take(dual_next, col, n_msgs, 0, d_rows, d_rows)
        away_ref[pl.ds(0, d_rows), :] = take(dual_next, col, n_msgs, half, d_rows, d_rows)

    @pl.when(jnp.logical_not(dual_core))
    def _():
        away_ref[pl.ds(0, p_rows), :] = primal_ref[pl.ds(DUAL * p_rows, p_rows), :]


def norm_body(n_msgs, p_total, d_total, *refs):
    msgs = by_offset(refs[:n_msgs], z_order(n_msgs))
    norm_out = refs[n_msgs]
    kept = norm_out.shape[1]

    @pl.when(jnp.logical_not(is_dual_core()))
    def _():
        def norms(squares, total):
            column = jnp.sqrt(jnp.sum(squares, axis=1, keepdims=True) / total)
            wide = jnp.broadcast_to(column, (kept, 128))
            row = lax.broadcasted_iota(jnp.int32, wide.shape, 0)
            lane = lax.broadcasted_iota(jnp.int32, wide.shape, 1)
            return jnp.sum(jnp.where(row == lane, wide, 0.0), axis=0, keepdims=True)[:, :kept]

        total = total_of(msgs, 2 * kept)
        norm_out[...] = jnp.concatenate(
            [norms(msgs[0][pl.ds(0, kept), :], p_total), norms(total[kept:], d_total)], axis=0
        )


def finish_body(dual_ref, primal_ref, back_ref, own_ref, got_ref, primal_out, dual_out, norm_out):
    width = dual_ref.shape[1]
    d_rows, p_rows = dual_out.shape[0] // width, primal_out.shape[0] // width
    dual_core = is_dual_core()

    def give(out_ref, rows):
        for r in range(rows.shape[0]):
            out_ref[pl.ds(r * width, width)] = rows[r]

    @pl.when(dual_core)
    def _():
        give(dual_out, dual_ref[...])
        give(primal_out, back_ref[pl.ds(0, p_rows), :])
        norm_out[...] = got_ref[...]

    @pl.when(jnp.logical_not(dual_core))
    def _():
        give(dual_out, back_ref[pl.ds(0, d_rows), :])
        give(primal_out, primal_ref[pl.ds((1 - DUAL) * p_rows, p_rows), :])
        norm_out[...] = own_ref[...]


def pack_body(n, *refs):
    (sources, out_ref, held, sem) = (refs[:n], refs[n], refs[n + 1 : 2 * n + 1], refs[2 * n + 1])
    copies = [
        pltpu.make_async_copy(source, ref, sem.at[i])
        for i, (source, ref) in enumerate(zip(sources, held, strict=True))
    ]
    for copy in copies:
        copy.start()
    for copy in copies:
        copy.wait()
    (cols_ref, *vectors) = held
    width = out_ref.shape[1]
    at = 0
    for ref in vectors:
        for i in range(ref.shape[0] // width):
            out_ref[at, :] = ref[pl.ds(i * width, width)]
            at += 1
    out_ref[pl.ds(at, cols_ref.shape[0]), pl.ds(0, cols_ref.shape[1])] = cols_ref[...].astype(F32)


def pack_call(out, *arrays):
    n = len(arrays)
    return pl.pallas_call(
        functools.partial(pack_body, n),
        out_shape=out,
        in_specs=[pl.BlockSpec(memory_space=pltpu.HBM)] * n,
        out_specs=pl.BlockSpec(memory_space=pltpu.VMEM),
        scratch_shapes=[pltpu.VMEM(a.shape, a.dtype) for a in arrays]
        + [pltpu.SemaphoreType.DMA((n,))],
        compiler_params=pltpu.CompilerParams(vmem_limit_bytes=66985984),
    )(*arrays)


def setup_body(d_rows, p_rows, slab_rows, slots, n_z, n_col, *refs):
    (own_ref, other_ref, dual_out, extra_out, cost_out, right_out, one_out, pick_out) = refs[:8]
    column_ref = refs[8]
    dual_core = is_dual_core()
    first = jnp.where(dual_core, own_ref[...], other_ref[...])
    second = jnp.where(dual_core, other_ref[...], own_ref[...])
    z, col = lax.axis_index("row") // 2, lax.axis_index("col")
    at = 0
    for slab, part in enumerate((first, second)):
        dual_out[pl.ds(slab * d_rows, d_rows), :] = part[:d_rows]
    at += d_rows
    for slab, part in enumerate((first, second)):
        piece = part[at : at + d_rows]
        for j in range(n_col):
            right_out[pl.ds(slab * slab_rows + j * d_rows, d_rows), :] = jnp.where(
                col == j, piece, 0.0
            )
    at += d_rows
    for slab, part in enumerate((first, second)):
        piece = part[at : at + p_rows]
        for j in range(n_z):
            cost_out[pl.ds((2 * j + slab ^ DUAL) * p_rows, p_rows), :] = jnp.where(
                z == j, piece, 0.0
            )
    at += p_rows
    for k in range(3):
        for slab, part in enumerate((first, second)):
            extra_out[pl.ds((2 * k + slab ^ DUAL) * p_rows, p_rows), :] = part[at : at + p_rows]
        at += p_rows
    entries, blocks = pick_out.shape
    side, lanes = -(-blocks // 128) * 128, column_ref.shape[1]
    column_ref[...] = jnp.full(column_ref.shape, -1.0, F32)
    for k, (part, slot) in enumerate((p, s) for p in (first, second) for s in range(slots)):
        column_ref[pl.ds(0, 1), pl.ds(k * slab_rows, slab_rows)] = part[
            at + slot : at + slot + 1, :slab_rows
        ]
    iota = lax.broadcasted_iota(jnp.int32, (side, lanes), 0).astype(F32)
    column = jnp.broadcast_to(column_ref[pl.ds(0, 1), :], (side, lanes))
    hot = jnp.where(column == iota, 1.0, 0.0)
    pick_out[...] = hot.T[:entries, :blocks].astype(BF16)
    one = hot[:blocks, :entries]
    one_out[...] = jnp.concatenate([one] * 3, axis=1).astype(BF16)


def primal_body(iteration, last, n_msgs, slots, *refs):
    msgs = by_offset(refs[:n_msgs], z_order(n_msgs))
    (primal_ref, low_ref, up_ref, hist_ref, right_ref, pick_ref, *blk_refs) = refs[
        n_msgs : n_msgs + 8
    ]
    (out_ref, primal_out, *rest) = refs[n_msgs + 8 :]
    blk_refs = blk_refs[::-1]
    blocks = primal_ref.shape[0]
    rows = right_ref.shape[0]
    slab_rows = rows // 2
    hist_out = out_ref.at[pl.ds(rows, hist_ref.shape[0])] if last else rest[0]
    bounds_out = rest[1:]

    @pl.when(jnp.logical_not(is_dual_core()))
    def _():
        total = total_of(msgs, blocks)
        if iteration == 0:
            each = blocks // n_msgs
            me = lax.axis_index("row") // 2
            for k, ref in enumerate((primal_out, *bounds_out)):
                parts = [m[pl.ds(blocks + k * each, each), :] for m in msgs]
                assemble(ref, parts, 0, each, each, me)
            primal, low, up = primal_out[...], bounds_out[0][...], bounds_out[1][...]
            hist_out[...] = jnp.zeros_like(hist_out)
        else:
            primal, low, up = primal_ref[...], low_ref[...], up_ref[...]
        primal_next = jnp.minimum(up, jnp.maximum(low, primal + STEP_PRIMAL * total))
        if last:
            index = lax.axis_index("row") // 2
            each = primal_out.shape[0]
            primal_out[...] = take(primal_next, index, n_msgs, 0, each, each)
        else:
            primal_out[...] = primal_next
        note_step(hist_out if iteration == 0 else hist_ref, hist_out, iteration, primal_next - primal)
        ext = (2.0 * primal_next - primal).astype(BF16)
        found = jnp.dot(pick_ref[...], ext, preferred_element_type=F32)
        picked = found.astype(BF16)
        by_vector = vector_rows(rows)
        turned = found.T if by_vector else None
        for r in range(rows):
            acc = -right_ref[pl.ds(r, 1), :]
            pairs = []
            for s in range(slots):
                at = (r // slab_rows * slots + s) * slab_rows + r % slab_rows
                block = blk_refs[r // slab_rows][r % slab_rows * slots + s]
                if r in by_vector:
                    pairs.append((block, turned[:, at : at + 1]))
                else:
                    acc = acc + jnp.dot(picked[at : at + 1], block, preferred_element_type=F32)
            if pairs:
                acc = acc + weigh(pairs)
            out_ref[pl.ds(r, 1), :] = acc


def weights_body(in_ref, out_ref, sem):
    copy = pltpu.make_async_copy(in_ref, out_ref, sem)
    copy.start()
    copy.wait()

    @pl.when(jnp.logical_not(is_dual_core()))
    def _():
        def step(i, carry):
            for k in range(16):
                out_ref[i * 16 + k] = out_ref[i * 16 + k].T
            return carry

        lax.fori_loop(0, in_ref.shape[0] // 16, step, 0)


def weights_call(blocks):
    return pl.pallas_call(
        weights_body,
        out_shape=jax.ShapeDtypeStruct(blocks.shape, BF16),
        in_specs=[pl.BlockSpec(memory_space=pltpu.HBM)],
        out_specs=pl.BlockSpec(memory_space=pltpu.VMEM),
        scratch_shapes=[pltpu.SemaphoreType.DMA],
        compiler_params=pltpu.CompilerParams(vmem_limit_bytes=8 * 2**20),
    )(blocks)


def local_call(body, outs, scratch, n_in):
    return pl.pallas_call(
        body,
        out_shape=outs,
        in_specs=[pl.BlockSpec(memory_space=pltpu.VMEM)] * n_in,
        out_specs=[pl.BlockSpec(memory_space=pltpu.VMEM)] * len(outs),
        scratch_shapes=scratch,
        compiler_params=pltpu.CompilerParams(vmem_limit_bytes=4 * 2**20),
    )


def per_device(
    blocks, block_cols, objective, lower_bound, upper_bound, right_side, primal_init, dual_init
):
    slab_rows, slots, width = blocks.shape[0], blocks.shape[1], blocks.shape[2]
    n_row, n_col = lax.axis_size("row"), lax.axis_size("col")
    n_z = n_row // 2
    p_rows = primal_init.shape[0] // width
    d_rows = dual_init.shape[0] // width
    col_blocks = p_rows * n_row
    rows = 2 * slab_rows
    entries = rows * slots

    swap_pairs = [(r, r ^ 1) for r in range(n_row)]

    def over_z(src, o):
        away = [(2 * k + src, 2 * (k ^ o) + 1 - src) for k in range(n_z)]
        return away + [(2 * k + 1 - src, 2 * k + src) for k in range(n_z)]

    def over_col(src, o):
        pairs = []
        for k in range(n_z):
            for c in range(n_col):
                pairs.append(((2 * k + src) * n_col + c, (2 * k + 1 - src) * n_col + (c ^ o)))
                pairs.append(((2 * k + 1 - src) * n_col + c, (2 * k + src) * n_col + c))
        return pairs

    def to_primal(x):
        return [lax.ppermute(x, "row", over_z(DUAL, o)) for o in z_order(n_z)]

    def to_dual(x):
        return [lax.ppermute(x, ("row", "col"), over_col(1 - DUAL, o)) for o in col_order(n_col)]

    def shape(n, wide=width, dtype=F32):
        return jax.ShapeDtypeStruct((n, wide), dtype)

    mine = blocks.reshape(slab_rows * slots, width, width)
    own = pack_call(
        shape(2 * d_rows + 4 * p_rows + slots),
        block_cols.T, dual_init, right_side, objective, primal_init, lower_bound, upper_bound,
    )
    gated, own = lax.optimization_barrier((mine, own))
    other = lax.ppermute(own, "row", swap_pairs)
    theirs = lax.ppermute(gated, "row", swap_pairs)
    dual_part, extra, cost, right, one_three, pick = local_call(
        functools.partial(setup_body, d_rows, p_rows, slab_rows, slots, n_z, n_col),
        [
            shape(2 * d_rows),
            shape(6 * p_rows),
            shape(col_blocks),
            shape(rows),
            shape(col_blocks, 3 * entries, BF16),
            shape(entries, col_blocks, BF16),
        ],
        [pltpu.VMEM((8, -(-entries // 128) * 128), F32)],
        2,
    )(own, other)
    own_weights = weights_call(mine)
    dual_part, own_weights = lax.optimization_barrier((dual_part, own_weights))
    weights = (own_weights, weights_call(theirs))

    hist_rows = -(-ITERS // 8) * 8
    dual = right
    primal = cost
    bounds = (cost, cost)
    primal_hist = dual_hist = jnp.zeros((hist_rows, width), F32)
    products = pltpu.VMEM((entries, width), F32)

    arrived = to_dual(dual_part)
    for iteration in range(ITERS):
        first, last = iteration == 0, iteration == ITERS - 1
        message, dual, dual_hist = local_call(
            functools.partial(dual_body, iteration, n_col, slots),
            [shape(col_blocks + (6 * p_rows if first else 0)), shape(rows), shape(hist_rows)],
            [products],
            n_col + 7,
        )(*arrived, dual, dual_hist, cost, one_three, extra, *weights)
        arrived = to_primal(message)
        message, primal, *others = local_call(
            functools.partial(primal_body, iteration, last, n_z, slots),
            [
                shape(rows + (hist_rows if last else 0)),
                shape(2 * p_rows if last else col_blocks),
            ]
            + [shape(hist_rows)] * (not last)
            + [shape(col_blocks)] * (2 if first else 0),
            [],
            n_z + 8,
        )(*arrived, primal, *bounds, primal_hist, right, pick, *weights)
        if first:
            bounds = others[1:]
        if not last:
            primal_hist = others[0]
        arrived = to_dual(message)
    message, dual, away = local_call(
        functools.partial(last_body, ITERS, n_col, d_rows, p_rows),
        [shape(2 * hist_rows), shape(d_rows), shape(max(p_rows, d_rows))],
        [pltpu.VMEM((rows, width), F32)],
        n_col + 3,
    )(*arrived, dual, dual_hist, primal)
    back = lax.ppermute(away, "row", swap_pairs)
    arrived = to_primal(message)
    (norms,) = local_call(
        functools.partial(
            norm_body,
            n_z,
            float(primal_init.shape[0] * n_row * n_col),
            float(dual_init.shape[0] * n_row * n_col),
        ),
        [shape(2, hist_rows)],
        [],
        n_z,
    )(*arrived)
    primal_out, dual_out, norms = local_call(
        finish_body,
        [
            jax.ShapeDtypeStruct(primal_init.shape, F32),
            jax.ShapeDtypeStruct(dual_init.shape, F32),
            shape(2, hist_rows),
        ],
        [],
        5,
    )(dual, primal, back, norms, lax.ppermute(norms, "row", swap_pairs))
    return (primal_out, dual_out, norms.T[:ITERS])


def solution(mesh):
    in_specs = (
        P("row", "col", None, None),
        P("row", "col"),
        P(("col", "row")),
        P(("col", "row")),
        P(("col", "row")),
        P(("row", "col")),
        P(("col", "row")),
        P(("row", "col")),
    )
    out_specs = (P(("col", "row")), P(("row", "col")), P())
    return jax.shard_map(
        per_device, mesh=mesh, in_specs=in_specs, out_specs=out_specs, check_vma=False
    )
```
